128 devices in a mesh: row: 8 (over y, core), col: 16 (over z, x).
Axes of the slice: x: 4, y: 4, z: 4, core: 2. Of those that a mesh axis runs over, the one named last changes fastest.
Arguments:
- images: bfloat16 [16384, 768], P(('row', 'col')), may hold values from -5 to 5
- texts: bfloat16 [16384, 768], P(('col', 'row')), may hold values from -5 to 5
- audio: bfloat16 [16384, 768], P(('col', 'row')), may hold values from -5 to 5
Outputs:
- grad_images: float32 [16384, 768], P(('row', 'col'))
- grad_texts: float32 [16384, 768], P(('col', 'row'))
- grad_audio: float32 [16384, 768], P(('col', 'row'))
The draws below stay inside these ranges and needn't reach their ends.
All inputs are finite; a program needn't handle non-finite values.
Results may differ from the reference program's by a relative error of at most 0.013.
Values may be sent and summed in bfloat16 or wider, within the bound.
A program may use at most 128 MiB of HBM per device.

```python
import math
import jax
import jax.numpy as jnp
from jax import lax

D = 768
ITERS = 3
BATCH = 16384


def paired(key, member):
    shared = jnp.clip(jax.random.normal(jax.random.fold_in(key, 101), (BATCH, D), jnp.float32), -6.0, 6.0)
    strength = jnp.exp(jax.random.uniform(jax.random.fold_in(key, 401), (BATCH, 1), jnp.float32, -1.2, 1.8))
    own_factor = jnp.exp(jax.random.uniform(jax.random.fold_in(key, 500 + member), (BATCH, 1), jnp.float32, -0.25, 0.25))
    spread = strength * own_factor
    jitter_key = jax.random.fold_in(key, 200 + member)
    jitter = jnp.clip(jax.random.normal(jitter_key, (BATCH, D), jnp.float32), -6.0, 6.0)
    mixed = (shared + spread * jitter) / jnp.sqrt(1.0 + spread * spread)
    return mixed / math.sqrt(D) * 0.8


def draw_images(key, part):
    return paired(key, 0).astype(jnp.bfloat16)


def draw_texts(key, part):
    return paired(key, 1).astype(jnp.bfloat16)


def draw_audio(key, part):
    return paired(key, 2).astype(jnp.bfloat16)


def setup_inputs(seed: int = 0) -> dict:
    seeds = jax.random.split(jax.random.key(seed), 4)
    images = draw_images(jax.random.fold_in(seeds[3], 71), 0)
    texts = draw_texts(jax.random.fold_in(seeds[3], 71), 0)
    audio = draw_audio(jax.random.fold_in(seeds[3], 71), 0)
    return dict(images=images, texts=texts, audio=audio)


logit_softness = 0.07
target_softness = 0.05
epsilon = 1e-06

def normalize(raw):
    values = raw.astype(jnp.float32)
    inverse = lax.rsqrt(lax.optimization_barrier(jnp.sum(values * values, axis=1, keepdims=True)) + epsilon)
    return (values * inverse, inverse)

def backward(unit, inverse, incoming):
    return (incoming - unit * lax.optimization_barrier(jnp.sum(unit * incoming, axis=1, keepdims=True))) * inverse

def score_gradient(cosine_matrix):
    loss_routine = jnp.exp(cosine_matrix / target_softness)
    cols_scale = jnp.ones((cosine_matrix.shape[1],), jnp.float32)
    rows_scale = jnp.ones((cosine_matrix.shape[0],), jnp.float32)
    for sweep in range(ITERS):
        rows_scale = 1.0 / lax.optimization_barrier(jnp.sum(loss_routine * cols_scale[None, :], axis=1))
        cols_scale = 1.0 / lax.optimization_barrier(jnp.sum(loss_routine * rows_scale[:, None], axis=0))
    target = loss_routine * rows_scale[:, None] * cols_scale[None, :]
    row_mass = lax.optimization_barrier(jnp.sum(target, axis=1))
    softmax_exponent = jnp.exp(cosine_matrix / logit_softness)
    row_total = lax.optimization_barrier(jnp.sum(softmax_exponent, axis=1))
    col_total = lax.optimization_barrier(jnp.sum(softmax_exponent, axis=0))
    score_grad = softmax_exponent / row_total[:, None] * row_mass[:, None] - target + softmax_exponent / col_total[None, :] - target
    return score_grad.astype(jnp.bfloat16)

def reference(images, texts, audio):
    img_unit, img_inverse = normalize(images)
    image_half_precision = img_unit.astype(jnp.bfloat16)
    image_gradient = jnp.zeros(img_unit.shape, jnp.float32)
    paired_out = []
    for modality in (texts, audio):
        unit, inverse = normalize(modality)
        unit_half_precision = unit.astype(jnp.bfloat16)
        cosine_matrix = lax.dot_general(image_half_precision, unit_half_precision, (((1,), (1,)), ((), ())), preferred_element_type=jnp.float32)
        score_matrix = score_gradient(cosine_matrix)
        image_gradient = image_gradient + jnp.dot(score_matrix, unit_half_precision, preferred_element_type=jnp.float32) / logit_softness
        other_gradient = lax.dot_general(score_matrix, image_half_precision, (((0,), (0,)), ((), ())), preferred_element_type=jnp.float32) / logit_softness
        paired_out.append(backward(unit, inverse, other_gradient))
    return (backward(img_unit, img_inverse, image_gradient), paired_out[0], paired_out[1])
```

```python
import functools

import jax
import jax.numpy as jnp
from jax import lax
from jax.experimental import pallas as pl
from jax.experimental.pallas import tpu as pltpu
from jax.sharding import PartitionSpec as P

ITERS = 3
logit_softness = 0.07
target_softness = 0.05
epsilon = 1e-06
LOG2E = 1.4426950408889634

MESH = pl.DeviceIdType.MESH
F32 = jnp.float32
BF16 = jnp.bfloat16
B = 128
D = 768
POS = [(2, 2), (1, 2), (3, 2), (0, 2), (2, 1), (2, 3), (2, 0), (1, 1), (1, 3), (3, 1), (3, 3), (0, 1), (0, 3), (1, 0), (3, 0), (0, 0)]
PI = {p: i for i, p in enumerate(POS)}
COLS = [(2, 0), (2, 1), (1, 0), (1, 1), (3, 0), (3, 1), (0, 0), (0, 1)]
CI = {p: i for i, p in enumerate(COLS)}
NSEM = 144


class Net:
    def __init__(self, send_sem, recv_sem):
        self.send_sem, self.recv_sem = send_sem, recv_sem
        self.index, self.sent = {}, []

    def at(self, tag):
        return self.index.setdefault(tag, len(self.index))

    def copy(self, tag, src, dst, device):
        i = self.at(tag)
        return pltpu.make_async_remote_copy(
            src_ref=src, dst_ref=dst, send_sem=self.send_sem.at[i], recv_sem=self.recv_sem.at[i],
            device_id=device, device_id_type=MESH,
        )

    def send(self, tag, src, dst, device):
        self.sent.append((tag, src, dst, device))
        self.make(tag, src, dst, device).start()

    def make(self, tag, src, dst, device):
        return self.copy(tag, src() if callable(src) else src, dst() if callable(dst) else dst, device)

    def wait(self, tag, landed, device):
        self.copy(tag, landed, landed, device).wait_recv()

    def drain(self):
        for entry in self.sent:
            self.make(*entry).wait_send()


def unit_of(raw_ref):
    values = raw_ref[...].astype(F32)
    inverse = lax.rsqrt(jnp.sum(values * values, axis=1, keepdims=True) + epsilon)
    return values * inverse, inverse


def lanes_to_rows(row):
    return jnp.broadcast_to(row, (B, B)).T


def kernel(
    img_in, txt_in, aud_in, out_img, out_txt, out_aud,
    img, cols, K, E, S,
    rows_local, rows_sent, rows_got, cols_local, cols_sent, cols_got, avec, bvec, rho, ict,
    st1, r1, st2, r2, st3, r3, st4, r4,
    gsib, sibgot, yst1, yr1, yst2, yr2,
    net_send, net_recv, rsend, rrecv, csend, crecv,
):
    row, col = lax.axis_index("row"), lax.axis_index("col")
    y, core = row // 2, lax.rem(row, 2)
    z, x = col // 4, lax.rem(col, 4)

    def wrap(v):
        return lax.rem(v, 4)

    def zx(dz, dx):
        return wrap(z + dz) * 4 + wrap(x + dx)

    def yc(dy, own):
        return wrap(y + dy) * 2 + (core if own else 1 - core)

    col_of = [zx(dz, dx) for dz, dx in POS]
    row_of = [yc(dy, own) for dy, own in COLS]

    def at_zx(dz, dx):
        return (row, col_of[PI[dz % 4, dx % 4]])

    def at_y(dy, own=1):
        return (row_of[CI[dy % 4, own]], col)

    barrier = pltpu.get_barrier_semaphore()
    for i in range(15):
        pl.semaphore_signal(barrier, inc=1, device_id=(row, col_of[i]), device_id_type=MESH)
    for i in range(7):
        pl.semaphore_signal(barrier, inc=1, device_id=(row_of[i], col), device_id_type=MESH)

    def image(dz, dx, start=0, count=B):
        return img.at[pl.ds(PI[dz % 4, dx % 4] * B + start, count), :]

    def column(m, dy, own, start=0, count=B):
        return cols.at[m, pl.ds(CI[dy % 4, own] * B + start, count), :]

    image(0, 0)[...] = unit_of(img_in)[0].astype(BF16)
    column(0, 0, 1)[...] = unit_of(txt_in)[0].astype(BF16)
    column(1, 0, 1)[...] = unit_of(aud_in)[0].astype(BF16)
    pl.semaphore_wait(barrier, 22)

    net = Net(net_send, net_recv)

    def place(h, first, second):
        return (first, second) if h == 0 else (second, first)

    def half_dev(h, first, second):
        return at_zx(*place(h, first, second))

    def first_send(h):
        for step in (1, 3):
            net.send(("g1", h, step), image(0, 0, 64 * h, 64), image(*place(h, -step, 0), 64 * h, 64), half_dev(h, step, 0))

    def second_send(h, f):
        for step in (1, 3):
            net.send(("g2", h, f, step), image(*place(h, f, 0), 64 * h, 64), image(*place(h, f, -step), 64 * h, 64), half_dev(h, 0, step))

    def first_forward(h, step):
        net.wait(("g1", h, step), image(*place(h, -step, 0), 64 * h, 64), half_dev(h, -step, 0))
        at = 64 * h + (0 if step == 1 else 32)
        net.send(("g1f", h, step), image(*place(h, -step, 0), at, 32), image(*place(h, 2, 0), at, 32), half_dev(h, step, 0))

    def first_end(h):
        for step in (1, 3):
            at = 64 * h + (0 if step == 1 else 32)
            net.wait(("g1f", h, step), image(*place(h, 2, 0), at, 32), half_dev(h, -step, 0))

    def second_forward(h, f):
        for step in (1, 3):
            net.wait(("g2", h, f, step), image(*place(h, f, -step), 64 * h, 64), half_dev(h, 0, -step))
            at = 64 * h + (0 if step == 1 else 32)
            net.send(("g2f", h, f, step), image(*place(h, f, -step), at, 32), image(*place(h, f, 2), at, 32), half_dev(h, 0, step))

    def second_end(h, f):
        for step in (1, 3):
            at = 64 * h + (0 if step == 1 else 32)
            net.wait(("g2f", h, f, step), image(*place(h, f, 2), at, 32), half_dev(h, 0, -step))

    def col_send(m):
        for step in (1, 3):
            net.send(("c1", m, step), column(m, 0, 1), column(m, -step, 1), at_y(step))
        net.send(("cs", m, 0), column(m, 0, 1), column(m, 0, 0), at_y(0, 0))

    def col_forward(m):
        for step in (1, 3):
            net.wait(("c1", m, step), column(m, -step, 1), at_y(-step))
            at = 0 if step == 1 else 64
            net.send(("c1f", m, step), column(m, -step, 1, at, 64), column(m, 2, 1, at, 64), at_y(step))
            net.send(("cs", m, -step % 4), column(m, -step, 1), column(m, -step, 0), at_y(0, 0))

    def col_end(m):
        for step in (1, 3):
            at = 0 if step == 1 else 64
            net.wait(("c1f", m, step), column(m, 2, 1, at, 64), at_y(-step))
        net.send(("cs", m, 2), column(m, 2, 1), column(m, 2, 0), at_y(0, 0))

    def col_rest(m):
        for dy in range(4):
            net.wait(("cs", m, dy), column(m, dy, 0), at_y(0, 0))

    for h in (0, 1):
        first_send(h)
    col_send(0)
    for h in (0, 1):
        second_send(h, 0)
    col_send(1)
    for step in (1, 3):
        for h in (0, 1):
            first_forward(h, step)
    for f in (3, 1):
        for h in (0, 1):
            second_send(h, f)
    col_forward(0)
    for h in (0, 1):
        second_forward(h, 0)
    for h in (0, 1):
        first_end(h)
        second_send(h, 2)
    for h in (0, 1):
        second_forward(h, 3)
    col_forward(1)
    col_end(0)
    for h in (0, 1):
        second_forward(h, 1)
    col_end(1)
    for h in (0, 1):
        second_forward(h, 2)
    for m in (0, 1):
        col_rest(m)
    for f in (0, 3, 1, 2):
        for h in (0, 1):
            second_end(h, f)

    def rows_send(k, m):
        for i in range(16):
            rows_sent[k, m, pl.ds(col_of[i], 1), :] = rows_local[m, i : i + 1, :]
        for i in range(15):
            pltpu.make_async_remote_copy(
                src_ref=rows_sent.at[k, m], dst_ref=rows_got.at[k, m, i], send_sem=rsend.at[k, m], recv_sem=rrecv.at[k, m],
                device_id=(row, col_of[i]), device_id_type=MESH,
            ).start()

    def rows_whole(k, m):
        return pltpu.make_async_remote_copy(
            src_ref=rows_got.at[k, m], dst_ref=rows_got.at[k, m], send_sem=rsend.at[k, m], recv_sem=rrecv.at[k, m],
            device_id=(row, col_of[0]), device_id_type=MESH,
        )

    def rows_sum(k, m):
        rows_whole(k, m).wait_recv()
        return rows_sent[k, m] + jnp.sum(rows_got[k, m], axis=0)

    def cols_send(k, m):
        for i in range(8):
            cols_sent[k, m, pl.ds(row_of[i], 1), :] = cols_local[m, i : i + 1, :]
        for i in range(7):
            pltpu.make_async_remote_copy(
                src_ref=cols_sent.at[k, m], dst_ref=cols_got.at[k, m, i], send_sem=csend.at[k, m], recv_sem=crecv.at[k, m],
                device_id=(row_of[i], col), device_id_type=MESH,
            ).start()

    def cols_whole(k, m):
        return pltpu.make_async_remote_copy(
            src_ref=cols_got.at[k, m], dst_ref=cols_got.at[k, m], send_sem=csend.at[k, m], recv_sem=crecv.at[k, m],
            device_id=(row_of[0], col), device_id_type=MESH,
        )

    def cols_sum(k, m):
        cols_whole(k, m).wait_recv()
        return cols_sent[k, m] + jnp.sum(cols_got[k, m], axis=0)

    def rows_back(dst, m, value):
        rows_local[m] = value
        for i in range(16):
            dst[m, i : i + 1, :] = rows_local[m, pl.ds(col_of[i], 1), :]

    def cols_back(dst, m, value):
        cols_local[m] = value
        for i in range(8):
            dst[m, i : i + 1, :] = cols_local[m, pl.ds(row_of[i], 1), :]

    def tile(j):
        return slice(j * B, (j + 1) * B)

    def row_part(part):
        return jnp.sum(part.T, axis=0, keepdims=True)

    def block(i):
        return pl.ds(pl.multiple_of(i * B, B), B)

    contract = (((1,), (1,)), ((), ()))

    def similarity(m):
        def body(i, carry):
            at = pl.ds(pl.multiple_of(i * 256, 256), 256)
            cosine = lax.dot_general(img[at, :], cols[m], contract, preferred_element_type=F32)
            E[m, at, :] = cosine
            part = jnp.zeros((256, B), F32)
            for j in range(8):
                kern = jnp.exp2(cosine[:, tile(j)] * (LOG2E / target_softness))
                K[m, at, tile(j)] = kern
                part = part + kern
            rows_local[m, pl.ds(2 * i, 1), :] = row_part(part[:B])
            rows_local[m, pl.ds(2 * i + 1, 1), :] = row_part(part[B:])
            return carry

        lax.fori_loop(0, 8, body, 0)

    def fold(value):
        return jnp.sum(value.reshape(16, 8, B), axis=0)

    def close_columns(m, acc):
        for j in range(8):
            cols_local[m, j : j + 1, :] = jnp.sum(acc[j], axis=0, keepdims=True)

    def softmax(m):
        def body(i, acc):
            part = jnp.zeros((B, B), F32)
            out = []
            for j in range(8):
                e = jnp.exp2(E[m, block(i), tile(j)] * (LOG2E / logit_softness))
                E[m, block(i), tile(j)] = e
                part = part + e
                out.append(acc[j] + fold(e))
            rows_local[m, pl.ds(i, 1), :] = row_part(part)
            return tuple(out)

        acc = lax.fori_loop(0, 16, body, tuple(jnp.zeros((8, B), F32) for _ in range(8)))
        close_columns(m, acc)

    def column_pass(m):
        def body(i, acc):
            a = lanes_to_rows(avec[m, pl.ds(i, 1), :])
            return tuple(acc[j] + fold(K[m, block(i), tile(j)] * a) for j in range(8))

        acc = lax.fori_loop(0, 16, body, tuple(jnp.zeros((8, B), F32) for _ in range(8)))
        close_columns(m, acc)

    def row_pass(m):
        def body(i, carry):
            part = K[m, block(i), tile(0)] * bvec[m, 0:1, :]
            for j in range(1, 8):
                part = part + K[m, block(i), tile(j)] * bvec[m, j : j + 1, :]
            rows_local[m, pl.ds(i, 1), :] = row_part(part)
            return carry

        lax.fori_loop(0, 16, body, 0)

    both = (0, 1)
    for m in both:
        similarity(m)
        rows_send(0, m)
    for m in both:
        softmax(m)
        rows_send(ITERS + 1, m)
        cols_send(ITERS, m)
    for sweep in range(ITERS):
        for m in both:
            rows_back(avec, m, 1.0 / rows_sum(sweep, m))
            column_pass(m)
            cols_send(sweep, m)
        for m in both:
            cols_back(bvec, m, 1.0 / cols_sum(sweep, m))
            row_pass(m)
            rows_send(sweep + 1, m)
    for m in both:
        cols_back(ict, m, 1.0 / cols_sum(ITERS, m))
    for m in both:
        rows_back(rho, m, rows_sum(ITERS, m) / rows_sum(ITERS + 1, m))

    for m in both:
        def score(i, carry, m=m):
            a = lanes_to_rows(avec[m, pl.ds(i, 1), :])
            mass = lanes_to_rows(avec[m, pl.ds(i, 1), :] * rho[m, pl.ds(i, 1), :])
            twice = a + a
            for j in range(8):
                soft = E[m, block(i), tile(j)] * (mass + ict[m, j : j + 1, :])
                target = K[m, block(i), tile(j)] * twice * bvec[m, j : j + 1, :]
                S[block(i), m * 1024 + j * B : m * 1024 + (j + 1) * B] = (soft - target).astype(BF16)
            return carry

        lax.fori_loop(0, 16, score, 0)

    def part_of(h, first, second, start=0, count=64):
        dz, dx = place(h, first % 4, second % 4)
        at = PI[dz, dx] * B + 64 * h + start
        return K[0, at : at + count, 0:D]

    def near_dev(h, step):
        return half_dev(h, 0, step)

    def far_dev(h, step):
        return half_dev(h, step, 0)

    def reduce1(h, f):
        st1[h, f] = part_of(h, f, 2).astype(BF16)
        for s, step in enumerate((1, 3)):
            net.send(
                ("r1", h, f, s), lambda s=s: st1.at[h, f, pl.ds(32 * s, 32), :], lambda s=s: r1.at[h, f, s], near_dev(h, step)
            )

    def reduce2(h, f, s):
        step = (1, 3)[s]
        net.wait(("r1", h, f, s), r1.at[h, f, s], near_dev(h, -step))
        for t in (0, 1):
            value = part_of(h, f, step, 32 * t, 32)
            if s == t:
                value = value + r1[h, f, s].astype(F32)
            st2[h, f, s, 32 * t : 32 * t + 32, :] = value.astype(BF16)
        net.send(("r2", h, f, s), lambda: st2.at[h, f, s], lambda: r2.at[h, f, s], near_dev(h, step))

    def line(h, f):
        for s, step in enumerate((1, 3)):
            net.wait(("r2", h, f, s), r2.at[h, f, s], near_dev(h, -step))
        return part_of(h, f, 0) + r2[h, f, 0].astype(F32) + r2[h, f, 1].astype(F32)

    def reduce3(h):
        st3[h] = line(h, 2).astype(BF16)
        for s, step in enumerate((1, 3)):
            net.send(("r3", h, s), st3.at[h, pl.ds(32 * s, 32), :], r3.at[h, s], far_dev(h, step))

    def reduce4(h, s):
        step = (1, 3)[s]
        value = line(h, step)
        net.wait(("r3", h, s), r3.at[h, s], far_dev(h, -step))
        for t in (0, 1):
            piece = value[32 * t : 32 * t + 32]
            if s == t:
                piece = piece + r3[h, s].astype(F32)
            st4[h, s, 32 * t : 32 * t + 32, :] = piece.astype(BF16)
        net.send(("r4", h, s), st4.at[h, s], r4.at[h, s], far_dev(h, step))

    def reduce5(h):
        value = line(h, 0)
        for s, step in enumerate((1, 3)):
            net.wait(("r4", h, s), r4.at[h, s], far_dev(h, -step))
        return value + r4[h, 0].astype(F32) + r4[h, 1].astype(F32)

    image_plan = {
        0: lambda: (reduce1(0, 2), reduce1(0, 1), reduce1(1, 2)),
        1: lambda: (reduce1(0, 3), reduce1(0, 0)),
        2: lambda: (reduce1(1, 1), reduce1(1, 3), reduce2(1, 2, 0), reduce2(1, 2, 1)),
        3: lambda: (reduce1(1, 0), reduce2(0, 2, 0), reduce2(0, 2, 1)),
        4: lambda: (reduce2(0, 1, 0), reduce2(0, 1, 1), reduce2(1, 1, 0), reduce2(1, 1, 1)),
        5: lambda: (reduce2(0, 3, 0), reduce2(0, 3, 1), reduce2(1, 3, 0), reduce2(1, 3, 1)),
        6: lambda: (reduce2(0, 0, 0), reduce2(0, 0, 1)),
        7: lambda: (reduce2(1, 0, 0), reduce2(1, 0, 1)),
    }

    def image_step(i, carry):
        at = pl.ds(pl.multiple_of(i * 256, 256), 256)
        total = jnp.dot(S[at, 0:1024], cols[0], preferred_element_type=F32)
        total = total + jnp.dot(S[at, 1024:2048], cols[1], preferred_element_type=F32)
        K[0, at, 0:D] = total
        for when, act in image_plan.items():
            @pl.when(i == when)
            def _(act=act):
                act()

        return carry

    lax.fori_loop(0, 8, image_step, 0)

    ORDER = (2, 1, 3, 0)

    def side_copy(m, k):
        return net.copy(("sib", m, k), gsib.at[m, k], sibgot.at[m, k], at_y(0, 0))

    def pair_sum(m, k):
        side_copy(m, k).wait_recv()
        at = (m * 4 + k) * B
        return K[1, at : at + B, 0:D] + sibgot[m, k].astype(F32)

    def ring1(m):
        yst1[m] = pair_sum(m, 0).astype(BF16)
        for s, step in enumerate((1, 3)):
            net.send(("y1", m, s), yst1.at[m, pl.ds(64 * s, 64), :], yr1.at[m, s], at_y(step))

    def ring2(m, s):
        step = (1, 3)[s]
        value = pair_sum(m, 1 + s)
        net.wait(("y1", m, s), yr1.at[m, s], at_y(-step))
        for t in (0, 1):
            piece = value[64 * t : 64 * t + 64]
            if s == t:
                piece = piece + yr1[m, s].astype(F32)
            yst2[m, s, 64 * t : 64 * t + 64, :] = piece.astype(BF16)
        net.send(("y2", m, s), yst2.at[m, s], yr2.at[m, s], at_y(step))

    def ring3(m):
        value = pair_sum(m, 3)
        for s, step in enumerate((1, 3)):
            net.wait(("y2", m, s), yr2.at[m, s], at_y(-step))
        return value + yr2[m, 0].astype(F32) + yr2[m, 1].astype(F32)

    column_plan = {
        1: lambda: (ring1(0), reduce3(0)),
        2: lambda: (ring1(1), reduce3(1)),
        4: lambda: (ring2(0, 0), reduce4(0, 0), reduce4(0, 1)),
        5: lambda: (ring2(1, 0), reduce4(1, 0), reduce4(1, 1)),
        6: lambda: (ring2(0, 1),),
        7: lambda: (ring2(1, 1),),
    }
    down = (((0,), (0,)), ((), ()))

    for k in range(4):
        for m in both:
            step = 2 * k + m
            total = lax.dot_general(
                S[:, m * 1024 + k * 256 : m * 1024 + k * 256 + 256], img[...], down, preferred_element_type=F32
            )
            gsib[m, k] = total[:B].astype(BF16)
            K[1, (m * 4 + k) * B : (m * 4 + k + 1) * B, 0:D] = total[B:]
            net.send(("sib", m, k), gsib.at[m, k], sibgot.at[m, k], at_y(0, 0))
            if step in column_plan:
                column_plan[step]()

    def finish(raw_ref, out_ref, rows, g):
        values = raw_ref[rows, :].astype(F32)
        inverse = lax.rsqrt(jnp.sum(values * values, axis=1, keepdims=True) + epsilon)
        unit = values * inverse
        g = g * (1.0 / logit_softness)
        out_ref[rows, :] = (g - unit * jnp.sum(unit * g, axis=1, keepdims=True)) * inverse

    for h in (0, 1):
        finish(img_in, out_img, slice(64 * h, 64 * h + 64), reduce5(h))
    finish(txt_in, out_txt, slice(0, B), ring3(0))
    finish(aud_in, out_aud, slice(0, B), ring3(1))

    net.drain()
    for m in both:
        for k in range(ITERS + 2):
            rows_whole(k, m).wait_send()
        for k in range(ITERS + 1):
            cols_whole(k, m).wait_send()


def shards(images, texts, audio):
    whole = pl.BlockSpec(memory_space=pltpu.VMEM)
    shape = jax.ShapeDtypeStruct(images.shape, F32)
    rounds_r, rounds_c = ITERS + 2, ITERS + 1
    return pl.pallas_call(
        kernel,
        out_shape=(shape, shape, shape),
        in_specs=[whole] * 3,
        out_specs=[whole] * 3,
        scratch_shapes=[
            pltpu.VMEM((2048, D), BF16),
            pltpu.VMEM((2, 1024, D), BF16),
            pltpu.VMEM((2, 2048, 1024), F32),
            pltpu.VMEM((2, 2048, 1024), F32),
            pltpu.VMEM((2048, 2048), BF16),
            pltpu.VMEM((2, 16, B), F32),
            pltpu.VMEM((rounds_r, 2, 16, B), F32),
            pltpu.VMEM((rounds_r, 2, 15, 16, B), F32),
            pltpu.VMEM((2, 8, B), F32),
            pltpu.VMEM((rounds_c, 2, 8, B), F32),
            pltpu.VMEM((rounds_c, 2, 7, 8, B), F32),
            pltpu.VMEM((2, 16, B), F32),
            pltpu.VMEM((2, 8, B), F32),
            pltpu.VMEM((2, 16, B), F32),
            pltpu.VMEM((2, 8, B), F32),
            pltpu.VMEM((2, 4, 64, D), BF16),
            pltpu.VMEM((2, 4, 2, 32, D), BF16),
            pltpu.VMEM((2, 4, 2, 64, D), BF16),
            pltpu.VMEM((2, 4, 2, 64, D), BF16),
            pltpu.VMEM((2, 64, D), BF16),
            pltpu.VMEM((2, 2, 32, D), BF16),
            pltpu.VMEM((2, 2, 64, D), BF16),
            pltpu.VMEM((2, 2, 64, D), BF16),
            pltpu.VMEM((2, 4, B, D), BF16),
            pltpu.VMEM((2, 4, B, D), BF16),
            pltpu.VMEM((2, B, D), BF16),
            pltpu.VMEM((2, 2, 64, D), BF16),
            pltpu.VMEM((2, 2, B, D), BF16),
            pltpu.VMEM((2, 2, B, D), BF16),
            pltpu.SemaphoreType.DMA((NSEM,)),
            pltpu.SemaphoreType.DMA((NSEM,)),
            pltpu.SemaphoreType.DMA((rounds_r, 2)),
            pltpu.SemaphoreType.DMA((rounds_r, 2)),
            pltpu.SemaphoreType.DMA((rounds_c, 2)),
            pltpu.SemaphoreType.DMA((rounds_c, 2)),
        ],
        compiler_params=pltpu.CompilerParams(
            collective_id=0, has_side_effects=True, vmem_limit_bytes=67043328
        ),
    )(images, texts, audio)


def solution(mesh):
    by_row = P(("row", "col"), None)
    by_col = P(("col", "row"), None)
    return jax.shard_map(
        shards,
        mesh=mesh,
        in_specs=(by_row, by_col, by_col),
        out_specs=(by_row, by_col, by_col),
        check_vma=False,
    )
```

```python
import functools

import jax
import jax.numpy as jnp
from jax import lax
from jax.experimental import pallas as pl
from jax.experimental.pallas import tpu as pltpu
from jax.sharding import PartitionSpec as P

ITERS = 3
logit_softness = 0.07
target_softness = 0.05
epsilon = 1e-06
LOG2E = 1.4426950408889634

MESH = pl.DeviceIdType.MESH
F32 = jnp.float32
BF16 = jnp.bfloat16
B = 128
D = 768
POS = [(2, 2), (1, 2), (3, 2), (0, 2), (2, 1), (2, 3), (2, 0), (1, 1), (1, 3), (3, 1), (3, 3), (0, 1), (0, 3), (1, 0), (3, 0), (0, 0)]
PI = {p: i for i, p in enumerate(POS)}
COLS = [(2, 0), (2, 1), (1, 0), (1, 1), (3, 0), (3, 1), (0, 0), (0, 1)]
CI = {p: i for i, p in enumerate(COLS)}
NSEM = 144
UNROLL = 4


class Net:
    def __init__(self, send_sem, recv_sem):
        self.send_sem, self.recv_sem = send_sem, recv_sem
        self.index, self.sent = {}, []

    def at(self, tag):
        return self.index.setdefault(tag, len(self.index))

    def copy(self, tag, src, dst, device):
        i = self.at(tag)
        return pltpu.make_async_remote_copy(
            src_ref=src, dst_ref=dst, send_sem=self.send_sem.at[i], recv_sem=self.recv_sem.at[i],
            device_id=device, device_id_type=MESH,
        )

    def send(self, tag, src, dst, device):
        self.sent.append((tag, src, dst, device))
        self.make(tag, src, dst, device).start()

    def make(self, tag, src, dst, device):
        return self.copy(tag, src() if callable(src) else src, dst() if callable(dst) else dst, device)

    def wait(self, tag, landed, device):
        self.copy(tag, landed, landed, device).wait_recv()

    def drain(self):
        for entry in self.sent:
            self.make(*entry).wait_send()


def unit_of(raw_ref):
    values = raw_ref[...].astype(F32)
    inverse = lax.rsqrt(jnp.sum(values * values, axis=1, keepdims=True) + epsilon)
    return values * inverse, inverse


def lanes_to_rows(row):
    return jnp.broadcast_to(row, (B, B)).T


def kernel(
    img_hbm, txt_hbm, aud_hbm, img_out, txt_out, aud_out,
    img_in, txt_in, aud_in, out_img, out_txt, out_aud, in_sem, out_sem,
    img, cols, K, E, S,
    rows_local, rows_turned, rows_sent, rows_got, cols_local, cols_sent, cols_got, avec, avec_turned, bvec, rho, ict, U,
    st1, r1, st2, r2, st3, r3, st4, r4,
    gsib, sibgot, yst1, yr1, yst2, yr2,
    net_send, net_recv, rsend, rrecv, csend, crecv,
):
    row, col = lax.axis_index("row"), lax.axis_index("col")
    y, core = row // 2, lax.rem(row, 2)
    z, x = col // 4, lax.rem(col, 4)

    def wrap(v):
        return lax.rem(v, 4)

    def zx(dz, dx):
        return wrap(z + dz) * 4 + wrap(x + dx)

    def yc(dy, own):
        return wrap(y + dy) * 2 + (core if own else 1 - core)

    col_of = [zx(dz, dx) for dz, dx in POS]
    row_of = [yc(dy, own) for dy, own in COLS]

    def at_zx(dz, dx):
        return (row, col_of[PI[dz % 4, dx % 4]])

    def at_y(dy, own=1):
        return (row_of[CI[dy % 4, own]], col)

    loads = [
        pltpu.make_async_copy(src, dst, in_sem.at[i])
        for i, (src, dst) in enumerate(((img_hbm, img_in), (txt_hbm, txt_in), (aud_hbm, aud_in)))
    ]
    for load in loads:
        load.start()

    barrier = pltpu.get_barrier_semaphore()
    near = [at_zx(1, 0), at_zx(3, 0), at_zx(0, 1), at_zx(0, 3), at_y(1), at_y(3), at_y(0, 0)]
    for device in near:
        pl.semaphore_signal(barrier, inc=1, device_id=device, device_id_type=MESH)

    def image(dz, dx, start=0, count=B):
        return img.at[pl.ds(PI[dz % 4, dx % 4] * B + start, count), :]

    def column(m, dy, own, start=0, count=B):
        return cols.at[pl.ds(m * 1024 + CI[dy % 4, own] * B + start, count), :]

    loads[0].wait()
    image(0, 0)[...] = unit_of(img_in)[0].astype(BF16)
    loads[1].wait()
    column(0, 0, 1)[...] = unit_of(txt_in)[0].astype(BF16)
    loads[2].wait()
    column(1, 0, 1)[...] = unit_of(aud_in)[0].astype(BF16)
    pl.semaphore_wait(barrier, len(near))

    net = Net(net_send, net_recv)

    def place(h, first, second):
        return (first, second) if h == 0 else (second, first)

    def half_dev(h, first, second):
        return at_zx(*place(h, first, second))

    def first_send(h):
        for step in (1, 3):
            net.send(("g1", h, step), image(0, 0, 64 * h, 64), image(*place(h, -step, 0), 64 * h, 64), half_dev(h, step, 0))

    def second_send(h, f):
        for step in (1, 3):
            net.send(("g2", h, f, step), image(*place(h, f, 0), 64 * h, 64), image(*place(h, f, -step), 64 * h, 64), half_dev(h, 0, step))

    def first_forward(h, step):
        net.wait(("g1", h, step), image(*place(h, -step, 0), 64 * h, 64), half_dev(h, -step, 0))
        at = 64 * h + (0 if step == 1 else 32)
        net.send(("g1f", h, step), image(*place(h, -step, 0), at, 32), image(*place(h, 2, 0), at, 32), half_dev(h, step, 0))

    def first_end(h):
        for step in (1, 3):
            at = 64 * h + (0 if step == 1 else 32)
            net.wait(("g1f", h, step), image(*place(h, 2, 0), at, 32), half_dev(h, -step, 0))

    def second_forward(h, f):
        for step in (1, 3):
            net.wait(("g2", h, f, step), image(*place(h, f, -step), 64 * h, 64), half_dev(h, 0, -step))
            at = 64 * h + (0 if step == 1 else 32)
            net.send(("g2f", h, f, step), image(*place(h, f, -step), at, 32), image(*place(h, f, 2), at, 32), half_dev(h, 0, step))

    def second_end(h, f):
        for step in (1, 3):
            at = 64 * h + (0 if step == 1 else 32)
            net.wait(("g2f", h, f, step), image(*place(h, f, 2), at, 32), half_dev(h, 0, -step))

    def col_send(m):
        for step in (1, 3):
            net.send(("c1", m, step), column(m, 0, 1), column(m, -step, 1), at_y(step))
        net.send(("cs", m, 0), column(m, 0, 1), column(m, 0, 0), at_y(0, 0))

    def col_forward(m):
        for step in (1, 3):
            net.wait(("c1", m, step), column(m, -step, 1), at_y(-step))
            at = 0 if step == 1 else 64
            net.send(("c1f", m, step), column(m, -step, 1, at, 64), column(m, 2, 1, at, 64), at_y(step))
            net.send(("cs", m, -step % 4), column(m, -step, 1), column(m, -step, 0), at_y(0, 0))

    def col_end(m):
        for step in (1, 3):
            at = 0 if step == 1 else 64
            net.wait(("c1f", m, step), column(m, 2, 1, at, 64), at_y(-step))
        net.send(("cs", m, 2), column(m, 2, 1), column(m, 2, 0), at_y(0, 0))

    def col_near(m):
        for dy in (0, 1, 3):
            net.wait(("cs", m, dy), column(m, dy, 0), at_y(0, 0))

    def col_far(m):
        net.wait(("cs", m, 2), column(m, 2, 0), at_y(0, 0))

    def tile(j):
        return slice(j * B, (j + 1) * B)

    def row_part(part):
        return jnp.sum(part.T, axis=0, keepdims=True)

    def block(i):
        return pl.ds(pl.multiple_of(i * B, B), B)

    contract = (((1,), (1,)), ((), ()))

    def similarity(m, lo, hi, left, right, first):
        def body(i, carry):
            at = pl.ds(pl.multiple_of(i * 256, 256), 256)
            cosine = lax.dot_general(
                img[at, :], cols[m * 1024 + left : m * 1024 + right, :], contract, preferred_element_type=F32
            )
            part = jnp.zeros((256, B), F32)
            for j in range((right - left) // B):
                piece = cosine[:, tile(j)]
                kern = jnp.exp2(piece * (LOG2E / target_softness))
                K[m, at, left + j * B : left + (j + 1) * B] = kern
                soft = jnp.exp2(piece * (LOG2E / logit_softness))
                E[at, m * 1024 + left + j * B : m * 1024 + left + (j + 1) * B] = soft.astype(BF16)
                part = part + kern
            for t in (0, 1):
                total = row_part(part[t * B : (t + 1) * B])
                if not first:
                    total = total + rows_local[m, pl.ds(2 * i + t, 1), :]
                rows_local[m, pl.ds(2 * i + t, 1), :] = total
            return carry

        lax.fori_loop(lo, hi, body, 0)

    for h in (0, 1):
        first_send(h)
    col_send(0)
    for h in (0, 1):
        second_send(h, 0)
    col_send(1)
    for step in (1, 3):
        for h in (0, 1):
            first_forward(h, step)
    for f in (3, 1):
        for h in (0, 1):
            second_send(h, f)
    col_forward(0)
    for h in (0, 1):
        second_forward(h, 0)
    for h in (0, 1):
        first_end(h)
        second_send(h, 2)
    col_near(0)
    similarity(0, 6, 8, 256, 1024, True)
    for h in (0, 1):
        second_forward(h, 3)
    col_forward(1)
    for h in (0, 1):
        second_forward(h, 1)
    col_near(1)
    similarity(1, 6, 8, 256, 1024, True)
    col_end(0)
    similarity(0, 4, 6, 256, 1024, True)
    for h in (0, 1):
        second_forward(h, 2)
    col_end(1)
    similarity(1, 4, 6, 256, 1024, True)
    for h in (0, 1):
        second_end(h, 0)
    for m in (0, 1):
        similarity(m, 3, 4, 256, 1024, True)
    for m in (0, 1):
        col_far(m)
        similarity(m, 3, 8, 0, 256, False)
    for f in (3, 1):
        for h in (0, 1):
            second_end(h, f)
    for m in (0, 1):
        similarity(m, 1, 3, 0, 1024, True)
    for h in (0, 1):
        second_end(h, 2)

    def rows_send(k, m):
        for i in range(16):
            rows_turned[m, pl.ds(col_of[i], 1), :] = rows_local[m, i : i + 1, :]
        rows_sent[k, m] = rows_turned[m].astype(BF16)
        for i in range(15):
            pltpu.make_async_remote_copy(
                src_ref=rows_sent.at[k, m], dst_ref=rows_got.at[k, m, i], send_sem=rsend.at[k, m], recv_sem=rrecv.at[k, m],
                device_id=(row, col_of[i]), device_id_type=MESH,
            ).start()

    def rows_whole(k, m):
        return pltpu.make_async_remote_copy(
            src_ref=rows_got.at[k, m], dst_ref=rows_got.at[k, m], send_sem=rsend.at[k, m], recv_sem=rrecv.at[k, m],
            device_id=(row, col_of[0]), device_id_type=MESH,
        )

    def rows_sum(k, m):
        rows_whole(k, m).wait_recv()
        return rows_sent[k, m].astype(F32) + jnp.sum(rows_got[k, m].astype(F32), axis=0)

    def cols_send(k, m):
        for i in range(8):
            cols_sent[k, m, pl.ds(row_of[i], 1), :] = cols_local[m, i : i + 1, :]
        for i in range(7):
            pltpu.make_async_remote_copy(
                src_ref=cols_sent.at[k, m], dst_ref=cols_got.at[k, m, i], send_sem=csend.at[k, m], recv_sem=crecv.at[k, m],
                device_id=(row_of[i], col), device_id_type=MESH,
            ).start()

    def cols_whole(k, m):
        return pltpu.make_async_remote_copy(
            src_ref=cols_got.at[k, m], dst_ref=cols_got.at[k, m], send_sem=csend.at[k, m], recv_sem=crecv.at[k, m],
            device_id=(row_of[0], col), device_id_type=MESH,
        )

    def cols_sum(k, m):
        cols_whole(k, m).wait_recv()
        return cols_sent[k, m] + jnp.sum(cols_got[k, m], axis=0)

    def rows_back(dst, m, value):
        rows_local[m] = value
        for i in range(16):
            dst[m, i : i + 1, :] = rows_local[m, pl.ds(col_of[i], 1), :]

    def cols_back(dst, m, value):
        cols_local[m] = value
        for i in range(8):
            dst[m, i : i + 1, :] = cols_local[m, pl.ds(row_of[i], 1), :]

    def fold(value):
        return jnp.sum(value.reshape(16, 8, B), axis=0)

    def close_columns(m, acc):
        for j in range(8):
            cols_local[m, j : j + 1, :] = jnp.sum(acc[j], axis=0, keepdims=True)

    def side(m, j):
        return slice(m * 1024 + j * B, m * 1024 + (j + 1) * B)

    zeros = tuple(jnp.zeros((8, B), F32) for _ in range(8))

    def over_blocks(one, carry):
        def body(t, carry):
            for u in range(UNROLL):
                carry = one(t * UNROLL + u, carry)
            return carry

        return lax.fori_loop(0, 16 // UNROLL, body, carry)

    def softmax(m):
        def one(i, acc):
            part = jnp.zeros((B, B), F32)
            out = []
            for j in range(8):
                e = E[block(i), side(m, j)].astype(F32)
                part = part + e
                out.append(acc[j] + fold(e))
            rows_local[m, pl.ds(i, 1), :] = row_part(part)
            return tuple(out)

        close_columns(m, over_blocks(one, zeros))

    def column_pass(m):
        def one(i, acc):
            a = lanes_to_rows(avec[m, pl.ds(i, 1), :])
            return tuple(acc[j] + fold(K[m, block(i), tile(j)] * a) for j in range(8))

        close_columns(m, over_blocks(one, zeros))

    def row_pass(m):
        def one(i, carry):
            part = K[m, block(i), tile(0)] * bvec[m, 0:1, :]
            for j in range(1, 8):
                part = part + K[m, block(i), tile(j)] * bvec[m, j : j + 1, :]
            rows_local[m, pl.ds(i, 1), :] = row_part(part)
            return carry

        over_blocks(one, 0)

    def soft_steps(lo, hi):
        def body(t, carry):
            m, i = t // 8, lax.rem(t, 8)
            at = pl.ds(pl.multiple_of(i * 256, 256), 256)
            here = pl.ds(pl.multiple_of(m * 1024, 1024), 1024)
            U[m, at, :] = jnp.dot(E[at, here], cols[here, :], preferred_element_type=F32).astype(BF16)
            return carry

        lax.fori_loop(lo, hi, body, 0)

    both = (0, 1)
    for m in both:
        similarity(m, 0, 1, 0, 1024, True)
        rows_send(0, m)
    for m in both:
        softmax(m)
        rows_send(ITERS + 1, m)
        cols_send(ITERS, m)
    cuts = [0, 3, 6, 9, 12, 16]
    for sweep in range(ITERS):
        for m in both:
            avec_turned[m] = 1.0 / rows_sum(sweep, m)
            rows_back(avec, m, avec_turned[m])
            column_pass(m)
            cols_send(sweep, m)
        soft_steps(cuts[2 * sweep], cuts[2 * sweep + 1])
        for m in both:
            cols_back(bvec, m, 1.0 / cols_sum(sweep, m))
            row_pass(m)
            rows_send(sweep + 1, m)
        if sweep < ITERS - 1:
            soft_steps(cuts[2 * sweep + 1], cuts[2 * sweep + 2])
    for m in both:
        cols_back(ict, m, 1.0 / cols_sum(ITERS, m))

    def score(i):
        for b in (2 * i, 2 * i + 1):
            at = slice(b * B, (b + 1) * B)
            for m in both:
                a = lanes_to_rows(avec[m, b : b + 1, :])
                twice = a + a
                for j in range(8):
                    soft = E[at, side(m, j)].astype(F32) * ict[m, j : j + 1, :]
                    target = K[m, at, tile(j)] * twice * bvec[m, j : j + 1, :]
                    S[at, side(m, j)] = (soft - target).astype(BF16)

    def whole_score(i):
        for b in (2 * i, 2 * i + 1):
            at = slice(b * B, (b + 1) * B)
            for m in both:
                mass = lanes_to_rows(rho[m, b : b + 1, :])
                for j in range(8):
                    soft = E[at, side(m, j)].astype(F32) * mass
                    E[at, side(m, j)] = (S[at, side(m, j)].astype(F32) + soft).astype(BF16)

    def part_of(h, first, second, start=0, count=64):
        dz, dx = place(h, first % 4, second % 4)
        at = PI[dz, dx] * B + 64 * h + start
        return K[0, at : at + count, 0:D]

    def near_dev(h, step):
        return half_dev(h, 0, step)

    def far_dev(h, step):
        return half_dev(h, step, 0)

    def reduce1(h, f):
        st1[h, f] = part_of(h, f, 2).astype(BF16)
        for s, step in enumerate((1, 3)):
            net.send(
                ("r1", h, f, s), lambda s=s: st1.at[h, f, pl.ds(32 * s, 32), :], lambda s=s: r1.at[h, f, s], near_dev(h, step)
            )

    def reduce2(h, f, s):
        step = (1, 3)[s]
        net.wait(("r1", h, f, s), r1.at[h, f, s], near_dev(h, -step))
        for t in (0, 1):
            value = part_of(h, f, step, 32 * t, 32)
            if s == t:
                value = value + r1[h, f, s].astype(F32)
            st2[h, f, s, 32 * t : 32 * t + 32, :] = value.astype(BF16)
        net.send(("r2", h, f, s), lambda: st2.at[h, f, s], lambda: r2.at[h, f, s], near_dev(h, step))

    def line(h, f):
        for s, step in enumerate((1, 3)):
            net.wait(("r2", h, f, s), r2.at[h, f, s], near_dev(h, -step))
        return part_of(h, f, 0) + r2[h, f, 0].astype(F32) + r2[h, f, 1].astype(F32)

    def reduce3(h):
        st3[h] = line(h, 2).astype(BF16)
        for s, step in enumerate((1, 3)):
            net.send(("r3", h, s), st3.at[h, pl.ds(32 * s, 32), :], r3.at[h, s], far_dev(h, step))

    def reduce4(h, s):
        step = (1, 3)[s]
        value = line(h, step)
        net.wait(("r3", h, s), r3.at[h, s], far_dev(h, -step))
        for t in (0, 1):
            piece = value[32 * t : 32 * t + 32]
            if s == t:
                piece = piece + r3[h, s].astype(F32)
            st4[h, s, 32 * t : 32 * t + 32, :] = piece.astype(BF16)
        net.send(("r4", h, s), st4.at[h, s], r4.at[h, s], far_dev(h, step))

    def reduce5(h):
        value = line(h, 0)
        for s, step in enumerate((1, 3)):
            net.wait(("r4", h, s), r4.at[h, s], far_dev(h, -step))
        return value + r4[h, 0].astype(F32) + r4[h, 1].astype(F32)

    def image_step(i, others):
        at = slice(i * 256, (i + 1) * 256)
        for n in range(3):
            out = slice(n * 256, (n + 1) * 256)
            total = jnp.dot(S[at, :], cols[:, out], preferred_element_type=F32)
            if n < len(others):
                others[n]()
            K[0, at, out] = total

    def add_soft(i):
        for b in (2 * i, 2 * i + 1):
            at = slice(b * B, (b + 1) * B)
            mass = [lanes_to_rows(rho[m, b : b + 1, :]) for m in both]
            for j in range(6):
                K[0, at, tile(j)] = (
                    K[0, at, tile(j)] + U[0, at, tile(j)].astype(F32) * mass[0] + U[1, at, tile(j)].astype(F32) * mass[1]
                )

    ORDER = (2, 1, 3, 0)

    def side_copy(m, k):
        return net.copy(("sib", m, k), gsib.at[m, k], sibgot.at[m, k], at_y(0, 0))

    def pair_sum(m, k):
        side_copy(m, k).wait_recv()
        at = (m * 4 + k) * B
        return K[1, at : at + B, 0:D] + sibgot[m, k].astype(F32)

    def ring1(m):
        yst1[m] = pair_sum(m, 0).astype(BF16)
        for s, step in enumerate((1, 3)):
            net.send(("y1", m, s), yst1.at[m, pl.ds(64 * s, 64), :], yr1.at[m, s], at_y(step))

    def ring2(m, s):
        step = (1, 3)[s]
        value = pair_sum(m, 1 + s)
        net.wait(("y1", m, s), yr1.at[m, s], at_y(-step))
        for t in (0, 1):
            piece = value[64 * t : 64 * t + 64]
            if s == t:
                piece = piece + yr1[m, s].astype(F32)
            yst2[m, s, 64 * t : 64 * t + 64, :] = piece.astype(BF16)
        net.send(("y2", m, s), yst2.at[m, s], yr2.at[m, s], at_y(step))

    def ring3(m):
        value = pair_sum(m, 3)
        for s, step in enumerate((1, 3)):
            net.wait(("y2", m, s), yr2.at[m, s], at_y(-step))
        return value + yr2[m, 0].astype(F32) + yr2[m, 1].astype(F32)

    down = (((0,), (0,)), ((), ()))

    def column_step(m, k):
        total = lax.dot_general(
            E[:, m * 1024 + k * 256 : m * 1024 + k * 256 + 256], img[...], down, preferred_element_type=F32
        )
        gsib[m, k] = total[:B].astype(BF16)
        K[1, (m * 4 + k) * B : (m * 4 + k + 1) * B, 0:D] = total[B:]
        net.send(("sib", m, k), gsib.at[m, k], sibgot.at[m, k], at_y(0, 0))

    def scores(*steps):
        return [functools.partial(score, i) for i in steps]

    def whole_scores(*steps):
        return [functools.partial(whole_score, i) for i in steps]

    score(0)
    image_step(0, scores(1, 2))
    image_step(1, scores(3, 4))
    image_step(2, scores(5, 6))
    image_step(3, scores(7))
    for m in both:
        rows_back(rho, m, avec_turned[m] * rows_sum(ITERS, m) / rows_sum(ITERS + 1, m))
    add_soft(0)
    reduce1(0, 2)
    reduce1(1, 2)
    reduce1(0, 1)
    add_soft(1)
    reduce1(0, 3)
    reduce1(0, 0)
    add_soft(2)
    reduce1(1, 1)
    reduce1(1, 3)
    add_soft(3)
    reduce1(1, 0)
    image_step(4, whole_scores(0, 1, 2))
    image_step(5, whole_scores(3, 4, 5))
    whole_score(6)
    whole_score(7)
    column_step(0, 0)
    add_soft(4)
    add_soft(5)
    for s in (0, 1):
        reduce2(0, 2, s)
        reduce2(1, 2, s)
    column_step(1, 0)
    ring1(0)
    for s in (0, 1):
        reduce2(0, 1, s)
        reduce2(1, 1, s)
    image_step(6, ())
    ring1(1)
    add_soft(6)
    for s in (0, 1):
        reduce2(0, 3, s)
        reduce2(1, 3, s)
    image_step(7, ())
    add_soft(7)
    for s in (0, 1):
        reduce2(0, 0, s)
        reduce2(1, 0, s)
    column_step(0, 1)
    column_step(0, 2)
    ring2(0, 0)
    reduce3(0)
    reduce3(1)
    column_step(1, 1)
    ring2(0, 1)
    column_step(1, 2)
    ring2(1, 0)
    for h in (0, 1):
        reduce4(h, 0)
    column_step(0, 3)
    ring2(1, 1)
    for h in (0, 1):
        reduce4(h, 1)
    column_step(1, 3)

    def finish(raw_ref, out_ref, rows, g):
        values = raw_ref[rows, :].astype(F32)
        inverse = lax.rsqrt(jnp.sum(values * values, axis=1, keepdims=True) + epsilon)
        unit = values * inverse
        g = g * (1.0 / logit_softness)
        out_ref[rows, :] = (g - unit * jnp.sum(unit * g, axis=1, keepdims=True)) * inverse

    stores = []

    def leave(src, dst):
        stores.append(pltpu.make_async_copy(src, dst, out_sem.at[len(stores)]))
        stores[-1].start()

    for h in (0, 1):
        finish(img_in, out_img, slice(64 * h, 64 * h + 64), reduce5(h))
    leave(out_img, img_out)
    finish(txt_in, out_txt, slice(0, B), ring3(0))
    leave(out_txt, txt_out)
    finish(aud_in, out_aud, slice(0, B), ring3(1))
    leave(out_aud, aud_out)

    net.drain()
    for m in both:
        for k in range(ITERS + 2):
            rows_whole(k, m).wait_send()
        for k in range(ITERS + 1):
            cols_whole(k, m).wait_send()
    for store in stores:
        store.wait()


def gradients(images, texts, audio):
    whole = pl.BlockSpec(memory_space=pl.ANY)
    shape = jax.ShapeDtypeStruct(images.shape, F32)
    rounds_r, rounds_c = ITERS + 2, ITERS + 1
    return pl.pallas_call(
        kernel,
        out_shape=(shape, shape, shape),
        in_specs=[whole] * 3,
        out_specs=[whole] * 3,
        scratch_shapes=[
            pltpu.VMEM((B, D), BF16),
            pltpu.VMEM((B, D), BF16),
            pltpu.VMEM((B, D), BF16),
            pltpu.VMEM((B, D), F32),
            pltpu.VMEM((B, D), F32),
            pltpu.VMEM((B, D), F32),
            pltpu.SemaphoreType.DMA((3,)),
            pltpu.SemaphoreType.DMA((3,)),
            pltpu.VMEM((2048, D), BF16),
            pltpu.VMEM((2048, D), BF16),
            pltpu.VMEM((2, 2048, 1024), F32),
            pltpu.VMEM((2048, 2048), BF16),
            pltpu.VMEM((2048, 2048), BF16),
            pltpu.VMEM((2, 16, B), F32),
            pltpu.VMEM((2, 16, B), F32),
            pltpu.VMEM((rounds_r, 2, 16, B), BF16),
            pltpu.VMEM((rounds_r, 2, 15, 16, B), BF16),
            pltpu.VMEM((2, 8, B), F32),
            pltpu.VMEM((rounds_c, 2, 8, B), F32),
            pltpu.VMEM((rounds_c, 2, 7, 8, B), F32),
            pltpu.VMEM((2, 16, B), F32),
            pltpu.VMEM((2, 16, B), F32),
            pltpu.VMEM((2, 8, B), F32),
            pltpu.VMEM((2, 16, B), F32),
            pltpu.VMEM((2, 8, B), F32),
            pltpu.VMEM((2, 2048, D), BF16),
            pltpu.VMEM((2, 4, 64, D), BF16),
            pltpu.VMEM((2, 4, 2, 32, D), BF16),
            pltpu.VMEM((2, 4, 2, 64, D), BF16),
            pltpu.VMEM((2, 4, 2, 64, D), BF16),
            pltpu.VMEM((2, 64, D), BF16),
            pltpu.VMEM((2, 2, 32, D), BF16),
            pltpu.VMEM((2, 2, 64, D), BF16),
            pltpu.VMEM((2, 2, 64, D), BF16),
            pltpu.VMEM((2, 4, B, D), BF16),
            pltpu.VMEM((2, 4, B, D), BF16),
            pltpu.VMEM((2, B, D), BF16),
            pltpu.VMEM((2, 2, 64, D), BF16),
            pltpu.VMEM((2, 2, B, D), BF16),
            pltpu.VMEM((2, 2, B, D), BF16),
            pltpu.SemaphoreType.DMA((NSEM,)),
            pltpu.SemaphoreType.DMA((NSEM,)),
            pltpu.SemaphoreType.DMA((rounds_r, 2)),
            pltpu.SemaphoreType.DMA((rounds_r, 2)),
            pltpu.SemaphoreType.DMA((rounds_c, 2)),
            pltpu.SemaphoreType.DMA((rounds_c, 2)),
        ],
        compiler_params=pltpu.CompilerParams(
            collective_id=0, has_side_effects=True, vmem_limit_bytes=67043328
        ),
    )(images, texts, audio)


def hand_over(a, b, c, x, y, z):
    x[...] = a[...]
    y[...] = b[...]
    z[...] = c[...]


def shards(images, texts, audio):
    outs = gradients(images, texts, audio)
    whole = pl.BlockSpec(memory_space=pltpu.VMEM)
    return pl.pallas_call(
        hand_over,
        out_shape=tuple(jax.ShapeDtypeStruct(o.shape, o.dtype) for o in outs),
        in_specs=[whole] * 3,
        out_specs=[whole] * 3,
    )(*outs)


def solution(mesh):
    by_row = P(("row", "col"), None)
    by_col = P(("col", "row"), None)
    return jax.shard_map(
        shards,
        mesh=mesh,
        in_specs=(by_row, by_col, by_col),
        out_specs=(by_row, by_col, by_col),
        check_vma=False,
    )
```

```python
import functools

import jax
import jax.numpy as jnp
from jax import lax
from jax.experimental import pallas as pl
from jax.experimental.pallas import tpu as pltpu
from jax.sharding import PartitionSpec as P

ITERS = 3
logit_softness = 0.07
target_softness = 0.05
epsilon = 1e-06
LOG2E = 1.4426950408889634

MESH = pl.DeviceIdType.MESH
F32 = jnp.float32
BF16 = jnp.bfloat16
B = 128
D = 768
POS = [(2, 2), (1, 2), (3, 2), (0, 2), (2, 1), (2, 3), (2, 0), (1, 1), (1, 3), (3, 1), (3, 3), (0, 1), (0, 3), (1, 0), (3, 0), (0, 0)]
PI = {p: i for i, p in enumerate(POS)}
COLS = [(2, 0), (2, 1), (1, 0), (1, 1), (3, 0), (3, 1), (0, 0), (0, 1)]
CI = {p: i for i, p in enumerate(COLS)}
NSEM = 144
UNROLL = 4


class Net:
    def __init__(self, send_sem, recv_sem):
        self.send_sem, self.recv_sem = send_sem, recv_sem
        self.index, self.sent = {}, []

    def at(self, tag):
        return self.index.setdefault(tag, len(self.index))

    def copy(self, tag, src, dst, device):
        i = self.at(tag)
        return pltpu.make_async_remote_copy(
            src_ref=src, dst_ref=dst, send_sem=self.send_sem.at[i], recv_sem=self.recv_sem.at[i],
            device_id=device, device_id_type=MESH,
        )

    def send(self, tag, src, dst, device):
        self.sent.append((tag, src, dst, device))
        self.make(tag, src, dst, device).start()

    def make(self, tag, src, dst, device):
        return self.copy(tag, src() if callable(src) else src, dst() if callable(dst) else dst, device)

    def wait(self, tag, landed, device):
        self.copy(tag, landed, landed, device).wait_recv()

    def drain(self):
        for entry in self.sent:
            self.make(*entry).wait_send()


def unit_of(raw_ref):
    values = raw_ref[...].astype(F32)
    inverse = lax.rsqrt(jnp.sum(values * values, axis=1, keepdims=True) + epsilon)
    return values * inverse, inverse


def lanes_to_rows(row):
    return jnp.broadcast_to(row, (B, B)).T


def kernel(
    img_hbm, txt_hbm, aud_hbm, img_out, txt_out, aud_out,
    img_in, txt_in, aud_in, out_img, out_txt, out_aud, in_sem, out_sem,
    img, cols, K, E, S,
    rows_local, rows_turned, rows_sent, rows_got, cols_local, cols_sent, cols_got, avec, avec_turned, bvec, rho, ict, U,
    st1, r1, st2, r2, st3, r3, st4, r4,
    gsib, sibgot, yst1, yr1, yst2, yr2,
    net_send, net_recv, rsend, rrecv, csend, crecv,
):
    row, col = lax.axis_index("row"), lax.axis_index("col")
    y, core = row // 2, lax.rem(row, 2)
    z, x = col // 4, lax.rem(col, 4)

    def wrap(v):
        return lax.rem(v, 4)

    def zx(dz, dx):
        return wrap(z + dz) * 4 + wrap(x + dx)

    def yc(dy, own):
        return wrap(y + dy) * 2 + (core if own else 1 - core)

    col_of = [zx(dz, dx) for dz, dx in POS]
    row_of = [yc(dy, own) for dy, own in COLS]

    def at_zx(dz, dx):
        return (row, col_of[PI[dz % 4, dx % 4]])

    def at_y(dy, own=1):
        return (row_of[CI[dy % 4, own]], col)

    loads = [
        pltpu.make_async_copy(src, dst, in_sem.at[i])
        for i, (src, dst) in enumerate(((img_hbm, img_in), (txt_hbm, txt_in), (aud_hbm, aud_in)))
    ]
    for load in loads:
        load.start()

    barrier = pltpu.get_barrier_semaphore()
    near = [at_zx(1, 0), at_zx(3, 0), at_zx(0, 1), at_zx(0, 3), at_y(1), at_y(3), at_y(0, 0)]
    for device in near:
        pl.semaphore_signal(barrier, inc=1, device_id=device, device_id_type=MESH)

    def image(dz, dx, start=0, count=B):
        return img.at[pl.ds(PI[dz % 4, dx % 4] * B + start, count), :]

    def column(m, dy, own, start=0, count=B):
        return cols.at[pl.ds(m * 1024 + CI[dy % 4, own] * B + start, count), :]

    loads[0].wait()
    image(0, 0)[...] = unit_of(img_in)[0].astype(BF16)
    loads[1].wait()
    column(0, 0, 1)[...] = unit_of(txt_in)[0].astype(BF16)
    loads[2].wait()
    column(1, 0, 1)[...] = unit_of(aud_in)[0].astype(BF16)
    pl.semaphore_wait(barrier, len(near))

    net = Net(net_send, net_recv)

    def place(h, first, second):
        return (first, second) if h == 0 else (second, first)

    def half_dev(h, first, second):
        return at_zx(*place(h, first, second))

    def first_send(h):
        for turn in (0, 1):
            for step in (1, 3):
                at = 64 * h + 32 * (turn if step == 1 else 1 - turn)
                net.send(("g1", h, step, turn), image(0, 0, at, 32), image(*place(h, -step, 0), at, 32), half_dev(h, step, 0))

    def first_landed(h, step, turn):
        at = 64 * h + 32 * (turn if step == 1 else 1 - turn)
        net.wait(("g1", h, step, turn), image(*place(h, -step, 0), at, 32), half_dev(h, -step, 0))

    def second_send(h, f):
        for step in (1, 3):
            net.send(("g2", h, f, step), image(*place(h, f, 0), 64 * h, 64), image(*place(h, f, -step), 64 * h, 64), half_dev(h, 0, step))

    def first_forward(h, step):
        first_landed(h, step, 0)
        at = 64 * h + (0 if step == 1 else 32)
        net.send(("g1f", h, step), image(*place(h, -step, 0), at, 32), image(*place(h, 2, 0), at, 32), half_dev(h, step, 0))

    def first_end(h):
        for step in (1, 3):
            at = 64 * h + (0 if step == 1 else 32)
            net.wait(("g1f", h, step), image(*place(h, 2, 0), at, 32), half_dev(h, -step, 0))

    def second_forward(h, f):
        for step in (1, 3):
            net.wait(("g2", h, f, step), image(*place(h, f, -step), 64 * h, 64), half_dev(h, 0, -step))
            at = 64 * h + (0 if step == 1 else 32)
            net.send(("g2f", h, f, step), image(*place(h, f, -step), at, 32), image(*place(h, f, 2), at, 32), half_dev(h, 0, step))

    def second_end(h, f):
        for step in (1, 3):
            at = 64 * h + (0 if step == 1 else 32)
            net.wait(("g2f", h, f, step), image(*place(h, f, 2), at, 32), half_dev(h, 0, -step))

    def col_at(step, turn):
        return 64 * (turn if step == 1 else 1 - turn)

    def col_send(m):
        for turn in (0, 1):
            for step in (1, 3):
                at = col_at(step, turn)
                net.send(("c1", m, step, turn), column(m, 0, 1, at, 64), column(m, -step, 1, at, 64), at_y(step))
        net.send(("cs", m, 0), column(m, 0, 1), column(m, 0, 0), at_y(0, 0))

    def col_landed(m, step, turn):
        net.wait(("c1", m, step, turn), column(m, -step, 1, col_at(step, turn), 64), at_y(-step))

    def col_forward(m):
        for step in (1, 3):
            col_landed(m, step, 0)
            at = col_at(step, 0)
            net.send(("c1f", m, step), column(m, -step, 1, at, 64), column(m, 2, 1, at, 64), at_y(step))

    def col_side(m):
        for step in (1, 3):
            col_landed(m, step, 1)
            net.send(("cs", m, -step % 4), column(m, -step, 1), column(m, -step, 0), at_y(0, 0))

    def col_end(m):
        for step in (1, 3):
            at = 0 if step == 1 else 64
            net.wait(("c1f", m, step), column(m, 2, 1, at, 64), at_y(-step))
        net.send(("cs", m, 2), column(m, 2, 1), column(m, 2, 0), at_y(0, 0))

    def col_near(m):
        for dy in (0, 1, 3):
            net.wait(("cs", m, dy), column(m, dy, 0), at_y(0, 0))

    def col_far(m):
        net.wait(("cs", m, 2), column(m, 2, 0), at_y(0, 0))

    def tile(j):
        return slice(j * B, (j + 1) * B)

    def row_part(part):
        return jnp.sum(part.T, axis=0, keepdims=True)

    def block(i):
        return pl.ds(pl.multiple_of(i * B, B), B)

    contract = (((1,), (1,)), ((), ()))

    def similarity(m, lo, hi, left, right, first, base=0, rows=256):
        def body(i, carry):
            at = pl.ds(pl.multiple_of(base + i * rows, B), rows)
            cosine = lax.dot_general(
                img[at, :], cols[m * 1024 + left : m * 1024 + right, :], contract, preferred_element_type=F32
            )
            for t in range(rows // B):
                here = pl.ds(pl.multiple_of(base + i * rows + t * B, B), B)
                part = jnp.zeros((B, B), F32)
                for j in range((right - left) // B):
                    piece = cosine[t * B : (t + 1) * B, tile(j)]
                    kern = jnp.exp2(piece * (LOG2E / target_softness))
                    K[m, here, left + j * B : left + (j + 1) * B] = kern
                    soft = jnp.exp2(piece * (LOG2E / logit_softness))
                    E[here, m * 1024 + left + j * B : m * 1024 + left + (j + 1) * B] = soft.astype(BF16)
                    part = part + kern
                total = row_part(part)
                line = pl.ds(base // B + i * (rows // B) + t, 1)
                if not first:
                    total = total + rows_local[m, line, :]
                rows_local[m, line, :] = total
            return carry

        lax.fori_loop(lo, hi, body, 0)

    for h in (0, 1):
        first_send(h)
    col_send(0)
    for h in (0, 1):
        second_send(h, 0)
    col_send(1)
    for step in (1, 3):
        for h in (0, 1):
            first_forward(h, step)
    for f, step in ((3, 1), (1, 3)):
        for h in (0, 1):
            first_landed(h, step, 1)
            second_send(h, f)
    col_forward(0)
    for h in (0, 1):
        second_forward(h, 0)
    for h in (0, 1):
        first_end(h)
        second_send(h, 2)
    col_side(0)
    col_near(0)
    similarity(0, 6, 8, 256, 1024, True)
    for h in (0, 1):
        second_forward(h, 3)
    col_forward(1)
    for h in (0, 1):
        second_forward(h, 1)
    col_side(1)
    col_near(1)
    similarity(1, 6, 8, 256, 1024, True)
    col_end(0)
    similarity(0, 4, 6, 256, 1024, True)
    for h in (0, 1):
        second_forward(h, 2)
    col_end(1)
    similarity(1, 4, 6, 256, 1024, True)
    for h in (0, 1):
        second_end(h, 0)
    for m in (0, 1):
        similarity(m, 3, 4, 256, 1024, True)
    for m in (0, 1):
        col_far(m)
        similarity(m, 0, 2, 0, 256, False, 768, 640)
    for f in (3, 1):
        for h in (0, 1):
            second_end(h, f)
    for m in (0, 1):
        similarity(m, 0, 1, 0, 1024, True, 256, 512)
    for h in (0, 1):
        second_end(h, 2)

    def rows_send(k, m):
        for i in range(16):
            rows_turned[m, pl.ds(col_of[i], 1), :] = rows_local[m, i : i + 1, :]
        rows_sent[k, m] = rows_turned[m].astype(BF16)
        for i in range(15):
            pltpu.make_async_remote_copy(
                src_ref=rows_sent.at[k, m], dst_ref=rows_got.at[k, m, i], send_sem=rsend.at[k, m], recv_sem=rrecv.at[k, m],
                device_id=(row, col_of[i]), device_id_type=MESH,
            ).start()

    def rows_whole(k, m):
        return pltpu.make_async_remote_copy(
            src_ref=rows_got.at[k, m], dst_ref=rows_got.at[k, m], send_sem=rsend.at[k, m], recv_sem=rrecv.at[k, m],
            device_id=(row, col_of[0]), device_id_type=MESH,
        )

    def rows_sum(k, m):
        rows_whole(k, m).wait_recv()
        return rows_sent[k, m].astype(F32) + jnp.sum(rows_got[k, m].astype(F32), axis=0)

    def cols_send(k, m):
        for i in range(8):
            cols_sent[k, m, pl.ds(row_of[i], 1), :] = cols_local[m, i : i + 1, :]
        for i in range(7):
            pltpu.make_async_remote_copy(
                src_ref=cols_sent.at[k, m], dst_ref=cols_got.at[k, m, i], send_sem=csend.at[k, m], recv_sem=crecv.at[k, m],
                device_id=(row_of[i], col), device_id_type=MESH,
            ).start()

    def cols_whole(k, m):
        return pltpu.make_async_remote_copy(
            src_ref=cols_got.at[k, m], dst_ref=cols_got.at[k, m], send_sem=csend.at[k, m], recv_sem=crecv.at[k, m],
            device_id=(row_of[0], col), device_id_type=MESH,
        )

    def cols_sum(k, m):
        cols_whole(k, m).wait_recv()
        return cols_sent[k, m] + jnp.sum(cols_got[k, m], axis=0)

    def rows_back(dst, m, value):
        rows_local[m] = value
        for i in range(16):
            dst[m, i : i + 1, :] = rows_local[m, pl.ds(col_of[i], 1), :]

    def cols_back(dst, m, value):
        cols_local[m] = value
        for i in range(8):
            dst[m, i : i + 1, :] = cols_local[m, pl.ds(row_of[i], 1), :]

    def fold(value):
        return jnp.sum(value.reshape(16, 8, B), axis=0)

    def close_columns(m, acc):
        for j in range(8):
            cols_local[m, j : j + 1, :] = jnp.sum(acc[j], axis=0, keepdims=True)

    def side(m, j):
        return slice(m * 1024 + j * B, m * 1024 + (j + 1) * B)

    zeros = tuple(jnp.zeros((8, B), F32) for _ in range(8))

    def over_blocks(one, carry):
        def body(t, carry):
            for u in range(UNROLL):
                carry = one(t * UNROLL + u, carry)
            return carry

        return lax.fori_loop(0, 16 // UNROLL, body, carry)

    def softmax(m):
        def one(i, acc):
            part = jnp.zeros((B, B), F32)
            out = []
            for j in range(8):
                e = E[block(i), side(m, j)].astype(F32)
                part = part + e
                out.append(acc[j] + fold(e))
            rows_local[m, pl.ds(i, 1), :] = row_part(part)
            return tuple(out)

        close_columns(m, over_blocks(one, zeros))

    def column_pass(m):
        def one(i, acc):
            a = lanes_to_rows(avec[m, pl.ds(i, 1), :])
            return tuple(acc[j] + fold(K[m, block(i), tile(j)] * a) for j in range(8))

        close_columns(m, over_blocks(one, zeros))

    def row_pass(m):
        def one(i, carry):
            part = K[m, block(i), tile(0)] * bvec[m, 0:1, :]
            for j in range(1, 8):
                part = part + K[m, block(i), tile(j)] * bvec[m, j : j + 1, :]
            rows_local[m, pl.ds(i, 1), :] = row_part(part)
            return carry

        over_blocks(one, 0)

    def soft_steps(lo, hi):
        def body(t, carry):
            m, i = t // 8, lax.rem(t, 8)
            at = pl.ds(pl.multiple_of(i * 256, 256), 256)
            here = pl.ds(pl.multiple_of(m * 1024, 1024), 1024)
            U[m, at, :] = jnp.dot(E[at, here], cols[here, :], preferred_element_type=F32).astype(BF16)
            return carry

        lax.fori_loop(lo, hi, body, 0)

    both = (0, 1)
    for m in both:
        similarity(m, 0, 1, 0, 1024, True)
        rows_send(0, m)
    for m in both:
        softmax(m)
        rows_send(ITERS + 1, m)
        cols_send(ITERS, m)
    cuts = [0, 3, 6, 9, 12, 16]
    for sweep in range(ITERS):
        for m in both:
            avec_turned[m] = 1.0 / rows_sum(sweep, m)
            rows_back(avec, m, avec_turned[m])
            column_pass(m)
            cols_send(sweep, m)
        soft_steps(cuts[2 * sweep], cuts[2 * sweep + 1])
        for m in both:
            cols_back(bvec, m, 1.0 / cols_sum(sweep, m))
            row_pass(m)
            rows_send(sweep + 1, m)
        if sweep < ITERS - 1:
            soft_steps(cuts[2 * sweep + 1], cuts[2 * sweep + 2])
    for m in both:
        cols_back(ict, m, 1.0 / cols_sum(ITERS, m))

    def score(i):
        for b in (2 * i, 2 * i + 1):
            at = slice(b * B, (b + 1) * B)
            for m in both:
                a = lanes_to_rows(avec[m, b : b + 1, :])
                twice = a + a
                for j in range(8):
                    soft = E[at, side(m, j)].astype(F32) * ict[m, j : j + 1, :]
                    target = K[m, at, tile(j)] * twice * bvec[m, j : j + 1, :]
                    S[at, side(m, j)] = (soft - target).astype(BF16)

    def whole_score(i):
        for b in (2 * i, 2 * i + 1):
            at = slice(b * B, (b + 1) * B)
            for m in both:
                mass = lanes_to_rows(rho[m, b : b + 1, :])
                for j in range(8):
                    soft = E[at, side(m, j)].astype(F32) * mass
                    E[at, side(m, j)] = (S[at, side(m, j)].astype(F32) + soft).astype(BF16)

    def part_of(h, first, second, start=0, count=64):
        dz, dx = place(h, first % 4, second % 4)
        at = PI[dz, dx] * B + 64 * h + start
        return K[0, at : at + count, 0:D]

    def near_dev(h, step):
        return half_dev(h, 0, step)

    def far_dev(h, step):
        return half_dev(h, step, 0)

    def reduce1(h, f):
        st1[h, f] = part_of(h, f, 2).astype(BF16)
        for s, step in enumerate((1, 3)):
            net.send(
                ("r1", h, f, s), lambda s=s: st1.at[h, f, pl.ds(32 * s, 32), :], lambda s=s: r1.at[h, f, s], near_dev(h, step)
            )

    def reduce2(h, f, s):
        step = (1, 3)[s]
        net.wait(("r1", h, f, s), r1.at[h, f, s], near_dev(h, -step))
        for t in (0, 1):
            value = part_of(h, f, step, 32 * t, 32)
            if s == t:
                value = value + r1[h, f, s].astype(F32)
            st2[h, f, s, 32 * t : 32 * t + 32, :] = value.astype(BF16)
        net.send(("r2", h, f, s), lambda: st2.at[h, f, s], lambda: r2.at[h, f, s], near_dev(h, step))

    def line(h, f):
        for s, step in enumerate((1, 3)):
            net.wait(("r2", h, f, s), r2.at[h, f, s], near_dev(h, -step))
        return part_of(h, f, 0) + r2[h, f, 0].astype(F32) + r2[h, f, 1].astype(F32)

    def reduce3(h):
        st3[h] = line(h, 2).astype(BF16)
        for s, step in enumerate((1, 3)):
            net.send(("r3", h, s), st3.at[h, pl.ds(32 * s, 32), :], r3.at[h, s], far_dev(h, step))

    def reduce4(h, s):
        step = (1, 3)[s]
        value = line(h, step)
        net.wait(("r3", h, s), r3.at[h, s], far_dev(h, -step))
        for t in (0, 1):
            piece = value[32 * t : 32 * t + 32]
            if s == t:
                piece = piece + r3[h, s].astype(F32)
            st4[h, s, 32 * t : 32 * t + 32, :] = piece.astype(BF16)
        net.send(("r4", h, s), st4.at[h, s], r4.at[h, s], far_dev(h, step))

    def reduce5(h):
        value = line(h, 0)
        for s, step in enumerate((1, 3)):
            net.wait(("r4", h, s), r4.at[h, s], far_dev(h, -step))
        return value + r4[h, 0].astype(F32) + r4[h, 1].astype(F32)

    def image_step(i, others):
        at = slice(i * 256, (i + 1) * 256)
        for other in others:
            other()
        K[0, at, 0:D] = jnp.dot(S[at, :], cols[...], preferred_element_type=F32)

    def add_soft(i):
        for b in (2 * i, 2 * i + 1):
            at = slice(b * B, (b + 1) * B)
            mass = [lanes_to_rows(rho[m, b : b + 1, :]) for m in both]
            for j in range(6):
                K[0, at, tile(j)] = (
                    K[0, at, tile(j)] + U[0, at, tile(j)].astype(F32) * mass[0] + U[1, at, tile(j)].astype(F32) * mass[1]
                )

    ORDER = (2, 1, 3, 0)

    def side_copy(m, k):
        return net.copy(("sib", m, k), gsib.at[m, k], sibgot.at[m, k], at_y(0, 0))

    def pair_sum(m, k):
        side_copy(m, k).wait_recv()
        at = (m * 4 + k) * B
        return K[1, at : at + B, 0:D] + sibgot[m, k].astype(F32)

    def ring1(m):
        yst1[m] = pair_sum(m, 0).astype(BF16)
        for s, step in enumerate((1, 3)):
            net.send(("y1", m, s), yst1.at[m, pl.ds(64 * s, 64), :], yr1.at[m, s], at_y(step))

    def ring2(m, s):
        step = (1, 3)[s]
        value = pair_sum(m, 1 + s)
        net.wait(("y1", m, s), yr1.at[m, s], at_y(-step))
        for t in (0, 1):
            piece = value[64 * t : 64 * t + 64]
            if s == t:
                piece = piece + yr1[m, s].astype(F32)
            yst2[m, s, 64 * t : 64 * t + 64, :] = piece.astype(BF16)
        net.send(("y2", m, s), yst2.at[m, s], yr2.at[m, s], at_y(step))

    def ring3(m):
        value = pair_sum(m, 3)
        for s, step in enumerate((1, 3)):
            net.wait(("y2", m, s), yr2.at[m, s], at_y(-step))
        return value + yr2[m, 0].astype(F32) + yr2[m, 1].astype(F32)

    down = (((0,), (0,)), ((), ()))

    def column_step(m, k):
        scored = E[:, m * 1024 + k * 256 : m * 1024 + k * 256 + 256]
        total = lax.dot_general(scored, img[...], down, preferred_element_type=F32)
        gsib[m, k] = total[:B].astype(BF16)
        K[1, (m * 4 + k) * B : (m * 4 + k + 1) * B, 0:D] = total[B:]
        net.send(("sib", m, k), gsib.at[m, k], sibgot.at[m, k], at_y(0, 0))

    def scores(*steps):
        return [functools.partial(score, i) for i in steps]

    def whole_scores(*steps):
        return [functools.partial(whole_score, i) for i in steps]

    score(0)
    image_step(0, scores(1, 2))
    image_step(1, scores(3, 4))
    image_step(2, scores(5, 6))
    image_step(3, scores(7))
    for m in both:
        rows_back(rho, m, avec_turned[m] * rows_sum(ITERS, m) / rows_sum(ITERS + 1, m))
    image_step(5, whole_scores(0, 1, 2))
    add_soft(2)
    add_soft(0)
    reduce1(0, 2)
    reduce1(1, 2)
    reduce1(0, 1)
    reduce1(1, 1)
    reduce1(1, 3)
    image_step(6, whole_scores(3, 4))
    add_soft(1)
    reduce1(0, 3)
    image_step(4, whole_scores(5, 6, 7))
    column_step(0, 0)
    reduce2(0, 2, 0)
    reduce2(0, 2, 1)
    reduce2(1, 2, 0)
    reduce2(1, 2, 1)
    column_step(0, 2)
    ring1(0)
    reduce1(0, 0)
    column_step(1, 0)
    add_soft(4)
    reduce2(1, 1, 1)
    reduce2(1, 3, 0)
    reduce2(0, 1, 1)
    column_step(0, 1)
    ring1(1)
    reduce2(0, 3, 0)
    add_soft(5)
    reduce2(0, 3, 1)
    add_soft(3)
    reduce1(1, 0)
    reduce2(0, 1, 0)
    reduce3(0)
    reduce2(1, 1, 0)
    column_step(1, 2)
    reduce3(1)
    ring2(0, 0)
    ring2(0, 1)
    reduce2(1, 3, 1)
    add_soft(6)
    reduce2(0, 0, 1)
    column_step(1, 3)
    column_step(1, 1)
    reduce2(1, 0, 0)
    ring2(1, 1)
    reduce2(0, 0, 0)
    image_step(7, whole_scores())
    add_soft(7)
    reduce4(0, 1)
    reduce2(1, 0, 1)
    ring2(1, 0)
    reduce4(0, 0)
    reduce4(1, 1)
    reduce4(1, 0)
    column_step(0, 3)

    def finish(raw_ref, out_ref, rows, g):
        values = raw_ref[rows, :].astype(F32)
        inverse = lax.rsqrt(jnp.sum(values * values, axis=1, keepdims=True) + epsilon)
        unit = values * inverse
        g = g * (1.0 / logit_softness)
        out_ref[rows, :] = (g - unit * jnp.sum(unit * g, axis=1, keepdims=True)) * inverse

    stores = []

    def leave(src, dst):
        stores.append(pltpu.make_async_copy(src, dst, out_sem.at[len(stores)]))
        stores[-1].start()

    finish(txt_in, out_txt, slice(0, B), ring3(0))
    leave(out_txt, txt_out)
    for h in (0, 1):
        finish(img_in, out_img, slice(64 * h, 64 * h + 64), reduce5(h))
    leave(out_img, img_out)
    finish(aud_in, out_aud, slice(0, B), ring3(1))
    leave(out_aud, aud_out)

    net.drain()
    for m in both:
        for k in range(ITERS + 2):
            rows_whole(k, m).wait_send()
        for k in range(ITERS + 1):
            cols_whole(k, m).wait_send()
    for store in stores:
        store.wait()


def gradients(images, texts, audio):
    whole = pl.BlockSpec(memory_space=pl.ANY)
    shape = jax.ShapeDtypeStruct(images.shape, F32)
    rounds_r, rounds_c = ITERS + 2, ITERS + 1
    return pl.pallas_call(
        kernel,
        out_shape=(shape, shape, shape),
        in_specs=[whole] * 3,
        out_specs=[whole] * 3,
        scratch_shapes=[
            pltpu.VMEM((B, D), BF16),
            pltpu.VMEM((B, D), BF16),
            pltpu.VMEM((B, D), BF16),
            pltpu.VMEM((B, D), F32),
            pltpu.VMEM((B, D), F32),
            pltpu.VMEM((B, D), F32),
            pltpu.SemaphoreType.DMA((3,)),
            pltpu.SemaphoreType.DMA((3,)),
            pltpu.VMEM((2048, D), BF16),
            pltpu.VMEM((2048, D), BF16),
            pltpu.VMEM((2, 2048, 1024), F32),
            pltpu.VMEM((2048, 2048), BF16),
            pltpu.VMEM((2048, 2048), BF16),
            pltpu.VMEM((2, 16, B), F32),
            pltpu.VMEM((2, 16, B), F32),
            pltpu.VMEM((rounds_r, 2, 16, B), BF16),
            pltpu.VMEM((rounds_r, 2, 15, 16, B), BF16),
            pltpu.VMEM((2, 8, B), F32),
            pltpu.VMEM((rounds_c, 2, 8, B), F32),
            pltpu.VMEM((rounds_c, 2, 7, 8, B), F32),
            pltpu.VMEM((2, 16, B), F32),
            pltpu.VMEM((2, 16, B), F32),
            pltpu.VMEM((2, 8, B), F32),
            pltpu.VMEM((2, 16, B), F32),
            pltpu.VMEM((2, 8, B), F32),
            pltpu.VMEM((2, 2048, D), BF16),
            pltpu.VMEM((2, 4, 64, D), BF16),
            pltpu.VMEM((2, 4, 2, 32, D), BF16),
            pltpu.VMEM((2, 4, 2, 64, D), BF16),
            pltpu.VMEM((2, 4, 2, 64, D), BF16),
            pltpu.VMEM((2, 64, D), BF16),
            pltpu.VMEM((2, 2, 32, D), BF16),
            pltpu.VMEM((2, 2, 64, D), BF16),
            pltpu.VMEM((2, 2, 64, D), BF16),
            pltpu.VMEM((2, 4, B, D), BF16),
            pltpu.VMEM((2, 4, B, D), BF16),
            pltpu.VMEM((2, B, D), BF16),
            pltpu.VMEM((2, 2, 64, D), BF16),
            pltpu.VMEM((2, 2, B, D), BF16),
            pltpu.VMEM((2, 2, B, D), BF16),
            pltpu.SemaphoreType.DMA((NSEM,)),
            pltpu.SemaphoreType.DMA((NSEM,)),
            pltpu.SemaphoreType.DMA((rounds_r, 2)),
            pltpu.SemaphoreType.DMA((rounds_r, 2)),
            pltpu.SemaphoreType.DMA((rounds_c, 2)),
            pltpu.SemaphoreType.DMA((rounds_c, 2)),
        ],
        compiler_params=pltpu.CompilerParams(
            collective_id=0, has_side_effects=True, vmem_limit_bytes=67043328
        ),
    )(images, texts, audio)


def hand_over(a, b, c, x, y, z):
    x[...] = a[...]
    y[...] = b[...]
    z[...] = c[...]


def shards(images, texts, audio):
    outs = gradients(images, texts, audio)
    whole = pl.BlockSpec(memory_space=pltpu.VMEM)
    return pl.pallas_call(
        hand_over,
        out_shape=tuple(jax.ShapeDtypeStruct(o.shape, o.dtype) for o in outs),
        in_specs=[whole] * 3,
        out_specs=[whole] * 3,
    )(*outs)


def solution(mesh):
    by_row = P(("row", "col"), None)
    by_col = P(("col", "row"), None)
    return jax.shard_map(
        shards,
        mesh=mesh,
        in_specs=(by_row, by_col, by_col),
        out_specs=(by_row, by_col, by_col),
        check_vma=False,
    )
```

```python
import functools

import jax
import jax.numpy as jnp
from jax import lax
from jax.experimental import pallas as pl
from jax.experimental.pallas import tpu as pltpu
from jax.sharding import PartitionSpec as P

ITERS = 3
logit_softness = 0.07
target_softness = 0.05
epsilon = 1e-06
LOG2E = 1.4426950408889634

MESH = pl.DeviceIdType.MESH
F32 = jnp.float32
BF16 = jnp.bfloat16
B = 128
D = 768
POS = [(2, 2), (1, 2), (3, 2), (0, 2), (2, 1), (2, 3), (2, 0), (1, 1), (1, 3), (3, 1), (3, 3), (0, 1), (0, 3), (1, 0), (3, 0), (0, 0)]
PI = {p: i for i, p in enumerate(POS)}
COLS = [(2, 0), (2, 1), (1, 0), (1, 1), (3, 0), (3, 1), (0, 0), (0, 1)]
CI = {p: i for i, p in enumerate(COLS)}
NSEM = 144
UNROLL = 4


class Net:
    def __init__(self, send_sem, recv_sem):
        self.send_sem, self.recv_sem = send_sem, recv_sem
        self.index, self.sent = {}, []

    def at(self, tag):
        return self.index.setdefault(tag, len(self.index))

    def copy(self, tag, src, dst, device):
        i = self.at(tag)
        return pltpu.make_async_remote_copy(
            src_ref=src, dst_ref=dst, send_sem=self.send_sem.at[i], recv_sem=self.recv_sem.at[i],
            device_id=device, device_id_type=MESH,
        )

    def send(self, tag, src, dst, device):
        self.sent.append((tag, src, dst, device))
        self.make(tag, src, dst, device).start()

    def make(self, tag, src, dst, device):
        return self.copy(tag, src() if callable(src) else src, dst() if callable(dst) else dst, device)

    def wait(self, tag, landed, device):
        self.copy(tag, landed, landed, device).wait_recv()

    def drain(self):
        for entry in self.sent:
            self.make(*entry).wait_send()


def unit_of(raw_ref):
    values = raw_ref[...].astype(F32)
    inverse = lax.rsqrt(jnp.sum(values * values, axis=1, keepdims=True) + epsilon)
    return values * inverse, inverse


def lanes_to_rows(row):
    return jnp.broadcast_to(row, (B, B)).T


def kernel(
    img_hbm, txt_hbm, aud_hbm, img_out, txt_out, aud_out,
    img_in, txt_in, aud_in, out_img, out_txt, out_aud, in_sem, out_sem,
    img, cols, K, E, S,
    rows_local, rows_turned, rows_sent, rows_got, cols_local, cols_sent, cols_got, avec, avec_turned, bvec, rho, ict, U,
    st1, r1, st2, r2, st3, r3, st4, r4,
    gsib, sibgot, yst1, yr1, yst2, yr2,
    net_send, net_recv, rsend, rrecv, csend, crecv,
):
    row, col = lax.axis_index("row"), lax.axis_index("col")
    y, core = row // 2, lax.rem(row, 2)
    z, x = col // 4, lax.rem(col, 4)

    def wrap(v):
        return lax.rem(v, 4)

    def zx(dz, dx):
        return wrap(z + dz) * 4 + wrap(x + dx)

    def yc(dy, own):
        return wrap(y + dy) * 2 + (core if own else 1 - core)

    col_of = [zx(dz, dx) for dz, dx in POS]
    row_of = [yc(dy, own) for dy, own in COLS]

    def at_zx(dz, dx):
        return (row, col_of[PI[dz % 4, dx % 4]])

    def at_y(dy, own=1):
        return (row_of[CI[dy % 4, own]], col)

    loads = [
        pltpu.make_async_copy(src, dst, in_sem.at[i])
        for i, (src, dst) in enumerate(((img_hbm, img_in), (txt_hbm, txt_in), (aud_hbm, aud_in)))
    ]
    for load in loads:
        load.start()

    barrier = pltpu.get_barrier_semaphore()
    near = [at_zx(1, 0), at_zx(3, 0), at_zx(0, 1), at_zx(0, 3), at_y(1), at_y(3), at_y(0, 0)]
    for device in near:
        pl.semaphore_signal(barrier, inc=1, device_id=device, device_id_type=MESH)

    def image(dz, dx, start=0, count=B):
        return img.at[pl.ds(PI[dz % 4, dx % 4] * B + start, count), :]

    def column(m, dy, own, start=0, count=B):
        return cols.at[pl.ds(m * 1024 + CI[dy % 4, own] * B + start, count), :]

    loads[0].wait()
    image(0, 0)[...] = unit_of(img_in)[0].astype(BF16)
    loads[1].wait()
    column(0, 0, 1)[...] = unit_of(txt_in)[0].astype(BF16)
    loads[2].wait()
    column(1, 0, 1)[...] = unit_of(aud_in)[0].astype(BF16)
    pl.semaphore_wait(barrier, len(near))

    net = Net(net_send, net_recv)

    def place(h, first, second):
        return (first, second) if h == 0 else (second, first)

    def half_dev(h, first, second):
        return at_zx(*place(h, first, second))

    def first_send(h):
        for turn in (0, 1):
            for step in (1, 3):
                at = 64 * h + 32 * (turn if step == 1 else 1 - turn)
                net.send(("g1", h, step, turn), image(0, 0, at, 32), image(*place(h, -step, 0), at, 32), half_dev(h, step, 0))

    def first_landed(h, step, turn):
        at = 64 * h + 32 * (turn if step == 1 else 1 - turn)
        net.wait(("g1", h, step, turn), image(*place(h, -step, 0), at, 32), half_dev(h, -step, 0))

    def second_send(h, f):
        for step in (1, 3):
            net.send(("g2", h, f, step), image(*place(h, f, 0), 64 * h, 64), image(*place(h, f, -step), 64 * h, 64), half_dev(h, 0, step))

    def first_forward(h, step):
        first_landed(h, step, 0)
        at = 64 * h + (0 if step == 1 else 32)
        net.send(("g1f", h, step), image(*place(h, -step, 0), at, 32), image(*place(h, 2, 0), at, 32), half_dev(h, step, 0))

    def first_end(h):
        for step in (1, 3):
            at = 64 * h + (0 if step == 1 else 32)
            net.wait(("g1f", h, step), image(*place(h, 2, 0), at, 32), half_dev(h, -step, 0))

    def second_forward(h, f):
        for step in (1, 3):
            net.wait(("g2", h, f, step), image(*place(h, f, -step), 64 * h, 64), half_dev(h, 0, -step))
            at = 64 * h + (0 if step == 1 else 32)
            net.send(("g2f", h, f, step), image(*place(h, f, -step), at, 32), image(*place(h, f, 2), at, 32), half_dev(h, 0, step))

    def second_end(h, f):
        for step in (1, 3):
            at = 64 * h + (0 if step == 1 else 32)
            net.wait(("g2f", h, f, step), image(*place(h, f, 2), at, 32), half_dev(h, 0, -step))

    def col_at(step, turn):
        return 64 * (turn if step == 1 else 1 - turn)

    def col_send(m):
        for turn in (0, 1):
            for step in (1, 3):
                at = col_at(step, turn)
                net.send(("c1", m, step, turn), column(m, 0, 1, at, 64), column(m, -step, 1, at, 64), at_y(step))
        net.send(("cs", m, 0), column(m, 0, 1), column(m, 0, 0), at_y(0, 0))

    def col_landed(m, step, turn):
        net.wait(("c1", m, step, turn), column(m, -step, 1, col_at(step, turn), 64), at_y(-step))

    def col_forward(m):
        for step in (1, 3):
            col_landed(m, step, 0)
            at = col_at(step, 0)
            net.send(("c1f", m, step), column(m, -step, 1, at, 64), column(m, 2, 1, at, 64), at_y(step))

    def col_side(m):
        for step in (1, 3):
            col_landed(m, step, 1)
            net.send(("cs", m, -step % 4), column(m, -step, 1), column(m, -step, 0), at_y(0, 0))

    def col_end(m):
        for step in (1, 3):
            at = 0 if step == 1 else 64
            net.wait(("c1f", m, step), column(m, 2, 1, at, 64), at_y(-step))
        net.send(("cs", m, 2), column(m, 2, 1), column(m, 2, 0), at_y(0, 0))

    def col_near(m):
        for dy in (0, 1, 3):
            net.wait(("cs", m, dy), column(m, dy, 0), at_y(0, 0))

    def col_far(m):
        net.wait(("cs", m, 2), column(m, 2, 0), at_y(0, 0))

    def tile(j):
        return slice(j * B, (j + 1) * B)

    def row_part(part):
        return jnp.sum(part.T, axis=0, keepdims=True)

    def block(i):
        return pl.ds(pl.multiple_of(i * B, B), B)

    contract = (((1,), (1,)), ((), ()))

    def similarity(m, lo, hi, left, right, first, base=0, rows=256):
        def body(i, carry):
            at = pl.ds(pl.multiple_of(base + i * rows, B), rows)
            cosine = lax.dot_general(
                img[at, :], cols[m * 1024 + left : m * 1024 + right, :], contract, preferred_element_type=F32
            )
            for t in range(rows // B):
                here = pl.ds(pl.multiple_of(base + i * rows + t * B, B), B)
                part = jnp.zeros((B, B), F32)
                for j in range((right - left) // B):
                    piece = cosine[t * B : (t + 1) * B, tile(j)]
                    kern = jnp.exp2(piece * (LOG2E / target_softness))
                    K[m, here, left + j * B : left + (j + 1) * B] = kern
                    soft = jnp.exp2(piece * (LOG2E / logit_softness))
                    E[here, m * 1024 + left + j * B : m * 1024 + left + (j + 1) * B] = soft.astype(BF16)
                    part = part + kern
                total = row_part(part)
                line = pl.ds(base // B + i * (rows // B) + t, 1)
                if not first:
                    total = total + rows_local[m, line, :]
                rows_local[m, line, :] = total
            return carry

        lax.fori_loop(lo, hi, body, 0)

    for h in (0, 1):
        first_send(h)
    col_send(0)
    for h in (0, 1):
        second_send(h, 0)
    col_send(1)
    for step in (1, 3):
        for h in (0, 1):
            first_forward(h, step)
    for f, step in ((3, 1), (1, 3)):
        for h in (0, 1):
            first_landed(h, step, 1)
            second_send(h, f)
    col_forward(0)
    for h in (0, 1):
        second_forward(h, 0)
    for h in (0, 1):
        first_end(h)
        second_send(h, 2)
    col_side(0)
    col_near(0)
    similarity(0, 6, 8, 256, 1024, True)
    for h in (0, 1):
        second_forward(h, 3)
    col_forward(1)
    for h in (0, 1):
        second_forward(h, 1)
    col_side(1)
    col_near(1)
    similarity(1, 6, 8, 256, 1024, True)
    col_end(0)
    similarity(0, 4, 6, 256, 1024, True)
    for h in (0, 1):
        second_forward(h, 2)
    col_end(1)
    similarity(1, 4, 6, 256, 1024, True)
    for h in (0, 1):
        second_end(h, 0)
    for m in (0, 1):
        similarity(m, 3, 4, 256, 1024, True)
    for m in (0, 1):
        col_far(m)
        similarity(m, 0, 2, 0, 256, False, 768, 640)
    for f in (3, 1):
        for h in (0, 1):
            second_end(h, f)
    for m in (0, 1):
        similarity(m, 0, 1, 0, 1024, True, 256, 512)
    for h in (0, 1):
        second_end(h, 2)

    def rows_send(k, m):
        for i in range(16):
            rows_turned[m, pl.ds(col_of[i], 1), :] = rows_local[m, i : i + 1, :]
        rows_sent[k, m] = rows_turned[m].astype(BF16)
        for i in range(15):
            pltpu.make_async_remote_copy(
                src_ref=rows_sent.at[k, m], dst_ref=rows_got.at[k, m, i], send_sem=rsend.at[k, m], recv_sem=rrecv.at[k, m],
                device_id=(row, col_of[i]), device_id_type=MESH,
            ).start()

    def rows_whole(k, m):
        return pltpu.make_async_remote_copy(
            src_ref=rows_got.at[k, m], dst_ref=rows_got.at[k, m], send_sem=rsend.at[k, m], recv_sem=rrecv.at[k, m],
            device_id=(row, col_of[0]), device_id_type=MESH,
        )

    def rows_sum(k, m):
        rows_whole(k, m).wait_recv()
        return rows_sent[k, m].astype(F32) + jnp.sum(rows_got[k, m].astype(F32), axis=0)

    def cols_send(k, m):
        for i in range(8):
            cols_sent[k, m, pl.ds(row_of[i], 1), :] = cols_local[m, i : i + 1, :]
        for i in range(7):
            pltpu.make_async_remote_copy(
                src_ref=cols_sent.at[k, m], dst_ref=cols_got.at[k, m, i], send_sem=csend.at[k, m], recv_sem=crecv.at[k, m],
                device_id=(row_of[i], col), device_id_type=MESH,
            ).start()

    def cols_whole(k, m):
        return pltpu.make_async_remote_copy(
            src_ref=cols_got.at[k, m], dst_ref=cols_got.at[k, m], send_sem=csend.at[k, m], recv_sem=crecv.at[k, m],
            device_id=(row_of[0], col), device_id_type=MESH,
        )

    def cols_sum(k, m):
        cols_whole(k, m).wait_recv()
        return cols_sent[k, m] + jnp.sum(cols_got[k, m], axis=0)

    def rows_back(dst, m, value):
        rows_local[m] = value
        for i in range(16):
            dst[m, i : i + 1, :] = rows_local[m, pl.ds(col_of[i], 1), :]

    def cols_back(dst, m, value):
        cols_local[m] = value
        for i in range(8):
            dst[m, i : i + 1, :] = cols_local[m, pl.ds(row_of[i], 1), :]

    def fold(value):
        return jnp.sum(value.reshape(16, 8, B), axis=0)

    def close_columns(m, acc):
        for j in range(8):
            cols_local[m, j : j + 1, :] = jnp.sum(acc[j], axis=0, keepdims=True)

    def side(m, j):
        return slice(m * 1024 + j * B, m * 1024 + (j + 1) * B)

    zeros = tuple(jnp.zeros((8, B), F32) for _ in range(8))

    def over_blocks(one, carry):
        def body(t, carry):
            for u in range(UNROLL):
                carry = one(t * UNROLL + u, carry)
            return carry

        return lax.fori_loop(0, 16 // UNROLL, body, carry)

    def softmax(m):
        def one(i, acc):
            part = jnp.zeros((B, B), F32)
            out = []
            for j in range(8):
                e = E[block(i), side(m, j)].astype(F32)
                part = part + e
                out.append(acc[j] + fold(e))
            rows_local[m, pl.ds(i, 1), :] = row_part(part)
            return tuple(out)

        close_columns(m, over_blocks(one, zeros))

    def column_pass(m):
        def one(i, acc):
            a = lanes_to_rows(avec[m, pl.ds(i, 1), :])
            return tuple(acc[j] + fold(K[m, block(i), tile(j)] * a) for j in range(8))

        close_columns(m, over_blocks(one, zeros))

    def row_pass(m):
        def one(i, carry):
            part = K[m, block(i), tile(0)] * bvec[m, 0:1, :]
            for j in range(1, 8):
                part = part + K[m, block(i), tile(j)] * bvec[m, j : j + 1, :]
            rows_local[m, pl.ds(i, 1), :] = row_part(part)
            return carry

        over_blocks(one, 0)

    def soft_steps(lo, hi):
        def body(t, carry):
            m, i = t // 8, lax.rem(t, 8)
            at = pl.ds(pl.multiple_of(i * 256, 256), 256)
            here = pl.ds(pl.multiple_of(m * 1024, 1024), 1024)
            U[m, at, :] = jnp.dot(E[at, here], cols[here, :], preferred_element_type=F32).astype(BF16)
            return carry

        lax.fori_loop(lo, hi, body, 0)

    both = (0, 1)
    for m in both:
        similarity(m, 0, 1, 0, 1024, True)
        rows_send(0, m)
    for m in both:
        softmax(m)
        rows_send(ITERS + 1, m)
        cols_send(ITERS, m)
    cuts = [0, 2, 6, 9, 13, 16]
    for sweep in range(ITERS):
        for m in both:
            avec_turned[m] = 1.0 / rows_sum(sweep, m)
            rows_back(avec, m, avec_turned[m])
            column_pass(m)
            cols_send(sweep, m)
        soft_steps(cuts[2 * sweep], cuts[2 * sweep + 1])
        for m in both:
            cols_back(bvec, m, 1.0 / cols_sum(sweep, m))
            row_pass(m)
            rows_send(sweep + 1, m)
        if sweep < ITERS - 1:
            soft_steps(cuts[2 * sweep + 1], cuts[2 * sweep + 2])
    for m in both:
        cols_back(ict, m, 1.0 / cols_sum(ITERS, m))

    def score(i):
        for b in (2 * i, 2 * i + 1):
            at = slice(b * B, (b + 1) * B)
            for m in both:
                a = lanes_to_rows(avec[m, b : b + 1, :])
                twice = a + a
                for j in range(8):
                    soft = E[at, side(m, j)].astype(F32) * ict[m, j : j + 1, :]
                    target = K[m, at, tile(j)] * twice * bvec[m, j : j + 1, :]
                    S[at, side(m, j)] = (soft - target).astype(BF16)

    def whole_score(i):
        for b in (2 * i, 2 * i + 1):
            at = slice(b * B, (b + 1) * B)
            for m in both:
                mass = lanes_to_rows(rho[m, b : b + 1, :])
                for j in range(8):
                    soft = E[at, side(m, j)].astype(F32) * mass
                    E[at, side(m, j)] = (S[at, side(m, j)].astype(F32) + soft).astype(BF16)

    def part_of(h, first, second, start=0, count=64):
        dz, dx = place(h, first % 4, second % 4)
        at = PI[dz, dx] * B + 64 * h + start
        return K[0, at : at + count, 0:D]

    def near_dev(h, step):
        return half_dev(h, 0, step)

    def far_dev(h, step):
        return half_dev(h, step, 0)

    def reduce1(h, f):
        st1[h, f] = part_of(h, f, 2).astype(BF16)
        for s, step in enumerate((1, 3)):
            net.send(
                ("r1", h, f, s), lambda s=s: st1.at[h, f, pl.ds(32 * s, 32), :], lambda s=s: r1.at[h, f, s], near_dev(h, step)
            )

    def reduce2(h, f, s):
        step = (1, 3)[s]
        net.wait(("r1", h, f, s), r1.at[h, f, s], near_dev(h, -step))
        for t in (0, 1):
            value = part_of(h, f, step, 32 * t, 32)
            if s == t:
                value = value + r1[h, f, s].astype(F32)
            st2[h, f, s, 32 * t : 32 * t + 32, :] = value.astype(BF16)
        net.send(("r2", h, f, s), lambda: st2.at[h, f, s], lambda: r2.at[h, f, s], near_dev(h, step))

    def line(h, f):
        for s, step in enumerate((1, 3)):
            net.wait(("r2", h, f, s), r2.at[h, f, s], near_dev(h, -step))
        return part_of(h, f, 0) + r2[h, f, 0].astype(F32) + r2[h, f, 1].astype(F32)

    def reduce3(h):
        st3[h] = line(h, 2).astype(BF16)
        for s, step in enumerate((1, 3)):
            net.send(("r3", h, s), st3.at[h, pl.ds(32 * s, 32), :], r3.at[h, s], far_dev(h, step))

    def reduce4(h, s):
        step = (1, 3)[s]
        value = line(h, step)
        net.wait(("r3", h, s), r3.at[h, s], far_dev(h, -step))
        for t in (0, 1):
            piece = value[32 * t : 32 * t + 32]
            if s == t:
                piece = piece + r3[h, s].astype(F32)
            st4[h, s, 32 * t : 32 * t + 32, :] = piece.astype(BF16)
        net.send(("r4", h, s), st4.at[h, s], r4.at[h, s], far_dev(h, step))

    def reduce5(h):
        value = line(h, 0)
        for s, step in enumerate((1, 3)):
            net.wait(("r4", h, s), r4.at[h, s], far_dev(h, -step))
        return value + r4[h, 0].astype(F32) + r4[h, 1].astype(F32)

    def image_step(i, others):
        at = slice(i * 256, (i + 1) * 256)
        for other in others:
            other()
        K[0, at, 0:D] = jnp.dot(S[at, :], cols[...], preferred_element_type=F32)

    def add_soft(i):
        for b in (2 * i, 2 * i + 1):
            at = slice(b * B, (b + 1) * B)
            mass = [lanes_to_rows(rho[m, b : b + 1, :]) for m in both]
            for j in range(6):
                K[0, at, tile(j)] = (
                    K[0, at, tile(j)] + U[0, at, tile(j)].astype(F32) * mass[0] + U[1, at, tile(j)].astype(F32) * mass[1]
                )

    ORDER = (2, 1, 3, 0)

    def side_copy(m, k):
        return net.copy(("sib", m, k), gsib.at[m, k], sibgot.at[m, k], at_y(0, 0))

    def pair_sum(m, k):
        side_copy(m, k).wait_recv()
        at = (m * 4 + k) * B
        return K[1, at : at + B, 0:D] + sibgot[m, k].astype(F32)

    def ring1(m):
        yst1[m] = pair_sum(m, 0).astype(BF16)
        for s, step in enumerate((1, 3)):
            net.send(("y1", m, s), yst1.at[m, pl.ds(64 * s, 64), :], yr1.at[m, s], at_y(step))

    def ring2(m, s):
        step = (1, 3)[s]
        value = pair_sum(m, 1 + s)
        net.wait(("y1", m, s), yr1.at[m, s], at_y(-step))
        for t in (0, 1):
            piece = value[64 * t : 64 * t + 64]
            if s == t:
                piece = piece + yr1[m, s].astype(F32)
            yst2[m, s, 64 * t : 64 * t + 64, :] = piece.astype(BF16)
        net.send(("y2", m, s), yst2.at[m, s], yr2.at[m, s], at_y(step))

    def ring3(m):
        value = pair_sum(m, 3)
        for s, step in enumerate((1, 3)):
            net.wait(("y2", m, s), yr2.at[m, s], at_y(-step))
        return value + yr2[m, 0].astype(F32) + yr2[m, 1].astype(F32)

    down = (((0,), (0,)), ((), ()))

    def column_step(m, k):
        scored = E[:, m * 1024 + k * 256 : m * 1024 + k * 256 + 256]
        total = lax.dot_general(scored, img[...], down, preferred_element_type=F32)
        gsib[m, k] = total[:B].astype(BF16)
        K[1, (m * 4 + k) * B : (m * 4 + k + 1) * B, 0:D] = total[B:]
        net.send(("sib", m, k), gsib.at[m, k], sibgot.at[m, k], at_y(0, 0))

    def scores(*steps):
        return [functools.partial(score, i) for i in steps]

    def whole_scores(*steps):
        return [functools.partial(whole_score, i) for i in steps]

    score(0)
    image_step(0, scores(1, 2))
    image_step(1, scores(3, 4))
    image_step(2, scores(5, 6))
    image_step(3, scores(7))
    for m in both:
        rows_back(rho, m, avec_turned[m] * rows_sum(ITERS, m) / rows_sum(ITERS + 1, m))
    image_step(5, whole_scores(0, 1, 2))
    add_soft(2)
    add_soft(0)
    reduce1(0, 2)
    reduce1(1, 2)
    reduce1(0, 1)
    reduce1(1, 1)
    reduce1(1, 3)
    image_step(6, whole_scores(3, 4))
    add_soft(1)
    reduce1(0, 3)
    image_step(4, whole_scores(5, 6, 7))
    column_step(0, 0)
    reduce2(0, 2, 0)
    reduce2(0, 2, 1)
    reduce2(1, 2, 0)
    reduce2(1, 2, 1)
    column_step(0, 2)
    ring1(0)
    reduce1(0, 0)
    column_step(1, 0)
    add_soft(4)
    reduce2(1, 1, 1)
    reduce2(1, 3, 0)
    reduce2(0, 1, 1)
    column_step(0, 1)
    ring1(1)
    reduce2(0, 3, 0)
    add_soft(5)
    reduce2(0, 3, 1)
    add_soft(3)
    reduce1(1, 0)
    reduce2(0, 1, 0)
    reduce3(0)
    reduce2(1, 1, 0)
    column_step(1, 2)
    reduce3(1)
    ring2(0, 0)
    ring2(0, 1)
    reduce2(1, 3, 1)
    add_soft(6)
    reduce2(0, 0, 1)
    column_step(1, 3)
    column_step(1, 1)
    reduce2(1, 0, 0)
    ring2(1, 1)
    reduce2(0, 0, 0)
    image_step(7, whole_scores())
    add_soft(7)
    reduce4(0, 1)
    reduce2(1, 0, 1)
    ring2(1, 0)
    reduce4(0, 0)
    reduce4(1, 1)
    reduce4(1, 0)
    column_step(0, 3)

    def finish(raw_ref, out_ref, rows, g):
        values = raw_ref[rows, :].astype(F32)
        inverse = lax.rsqrt(jnp.sum(values * values, axis=1, keepdims=True) + epsilon)
        unit = values * inverse
        g = g * (1.0 / logit_softness)
        out_ref[rows, :] = (g - unit * jnp.sum(unit * g, axis=1, keepdims=True)) * inverse

    stores = []

    def leave(src, dst):
        stores.append(pltpu.make_async_copy(src, dst, out_sem.at[len(stores)]))
        stores[-1].start()

    finish(txt_in, out_txt, slice(0, B), ring3(0))
    leave(out_txt, txt_out)
    for h in (0, 1):
        finish(img_in, out_img, slice(64 * h, 64 * h + 64), reduce5(h))
    leave(out_img, img_out)
    finish(aud_in, out_aud, slice(0, B), ring3(1))
    leave(out_aud, aud_out)

    net.drain()
    for m in both:
        for k in range(ITERS + 2):
            rows_whole(k, m).wait_send()
        for k in range(ITERS + 1):
            cols_whole(k, m).wait_send()
    for store in stores:
        store.wait()


def gradients(images, texts, audio):
    whole = pl.BlockSpec(memory_space=pl.ANY)
    shape = jax.ShapeDtypeStruct(images.shape, F32)
    rounds_r, rounds_c = ITERS + 2, ITERS + 1
    return pl.pallas_call(
        kernel,
        out_shape=(shape, shape, shape),
        in_specs=[whole] * 3,
        out_specs=[whole] * 3,
        scratch_shapes=[
            pltpu.VMEM((B, D), BF16),
            pltpu.VMEM((B, D), BF16),
            pltpu.VMEM((B, D), BF16),
            pltpu.VMEM((B, D), F32),
            pltpu.VMEM((B, D), F32),
            pltpu.VMEM((B, D), F32),
            pltpu.SemaphoreType.DMA((3,)),
            pltpu.SemaphoreType.DMA((3,)),
            pltpu.VMEM((2048, D), BF16),
            pltpu.VMEM((2048, D), BF16),
            pltpu.VMEM((2, 2048, 1024), F32),
            pltpu.VMEM((2048, 2048), BF16),
            pltpu.VMEM((2048, 2048), BF16),
            pltpu.VMEM((2, 16, B), F32),
            pltpu.VMEM((2, 16, B), F32),
            pltpu.VMEM((rounds_r, 2, 16, B), BF16),
            pltpu.VMEM((rounds_r, 2, 15, 16, B), BF16),
            pltpu.VMEM((2, 8, B), F32),
            pltpu.VMEM((rounds_c, 2, 8, B), F32),
            pltpu.VMEM((rounds_c, 2, 7, 8, B), F32),
            pltpu.VMEM((2, 16, B), F32),
            pltpu.VMEM((2, 16, B), F32),
            pltpu.VMEM((2, 8, B), F32),
            pltpu.VMEM((2, 16, B), F32),
            pltpu.VMEM((2, 8, B), F32),
            pltpu.VMEM((2, 2048, D), BF16),
            pltpu.VMEM((2, 4, 64, D), BF16),
            pltpu.VMEM((2, 4, 2, 32, D), BF16),
            pltpu.VMEM((2, 4, 2, 64, D), BF16),
            pltpu.VMEM((2, 4, 2, 64, D), BF16),
            pltpu.VMEM((2, 64, D), BF16),
            pltpu.VMEM((2, 2, 32, D), BF16),
            pltpu.VMEM((2, 2, 64, D), BF16),
            pltpu.VMEM((2, 2, 64, D), BF16),
            pltpu.VMEM((2, 4, B, D), BF16),
            pltpu.VMEM((2, 4, B, D), BF16),
            pltpu.VMEM((2, B, D), BF16),
            pltpu.VMEM((2, 2, 64, D), BF16),
            pltpu.VMEM((2, 2, B, D), BF16),
            pltpu.VMEM((2, 2, B, D), BF16),
            pltpu.SemaphoreType.DMA((NSEM,)),
            pltpu.SemaphoreType.DMA((NSEM,)),
            pltpu.SemaphoreType.DMA((rounds_r, 2)),
            pltpu.SemaphoreType.DMA((rounds_r, 2)),
            pltpu.SemaphoreType.DMA((rounds_c, 2)),
            pltpu.SemaphoreType.DMA((rounds_c, 2)),
        ],
        compiler_params=pltpu.CompilerParams(
            collective_id=0, has_side_effects=True, vmem_limit_bytes=67043328
        ),
    )(images, texts, audio)


def hand_over(a, b, c, x, y, z):
    x[...] = a[...]
    y[...] = b[...]
    z[...] = c[...]


def shards(images, texts, audio):
    outs = gradients(images, texts, audio)
    whole = pl.BlockSpec(memory_space=pltpu.VMEM)
    return pl.pallas_call(
        hand_over,
        out_shape=tuple(jax.ShapeDtypeStruct(o.shape, o.dtype) for o in outs),
        in_specs=[whole] * 3,
        out_specs=[whole] * 3,
    )(*outs)


def solution(mesh):
    by_row = P(("row", "col"), None)
    by_col = P(("col", "row"), None)
    return jax.shard_map(
        shards,
        mesh=mesh,
        in_specs=(by_row, by_col, by_col),
        out_specs=(by_row, by_col, by_col),
        check_vma=False,
    )
```
